32 devices in a mesh: fsdp: 4 (over x, core), ep: 8 (over z, y).
Axes of the slice: x: 2, y: 2, z: 4, core: 2. Of those that a mesh axis runs over, the one named last changes fastest.
Arguments:
- tokens: bfloat16 [256, 2048], P(('fsdp', 'ep')), may hold values from -6 to 6
- cotangent: bfloat16 [256, 2048], P(('fsdp', 'ep')), may hold values from -4 to 4
- routes: int32 [256, 2], P(('fsdp', 'ep')), may hold values from 0 to 7, as said below
- logits: float32 [256, 8], P(('fsdp', 'ep')), may hold values from -8 to 8
- w_gate: bfloat16 [2048, 16384], P('fsdp', 'ep'), may hold values from -0.125 to 0.125
- w_up: bfloat16 [2048, 16384], P('fsdp', 'ep'), may hold values from -0.125 to 0.125
- w_down: bfloat16 [16384, 2048], P('ep', 'fsdp'), may hold values from -0.0625 to 0.0625
Outputs:
- grad_tokens: bfloat16 [256, 2048], P(('fsdp', 'ep'))
- route_dot: float32 [256, 2], P(('fsdp', 'ep'))
- aux_grad: float32 [256, 8], P(('fsdp', 'ep'))
- grad_gate: bfloat16 [2048, 16384], P('fsdp', 'ep')
- grad_up: bfloat16 [2048, 16384], P('fsdp', 'ep')
- grad_down: bfloat16 [16384, 2048], P('ep', 'fsdp')
The draws below stay inside these ranges and needn't reach their ends.
Inputs may be any that keep to these rules, and one draw needn't show every extreme that they name: `routes`: each token names two different experts; on every device at most 3 tokens name one expert, and some expert is named by exactly 3 of them.
All inputs are finite; a program needn't handle non-finite values.
Results may differ from the reference program's by a relative error of at most 0.04.
Values may be sent and summed in bfloat16 or wider, within the bound.
A program may use at most 128 MiB of HBM per device.

```python
import jax
import jax.numpy as jnp
from jax import lax

D = 2048
FF = 8192
EXPERTS = 8
EXP_WIN = 2
TOK_DEV = 8
CAP = 3
TOKENS = 256
N_FSDP = 4
N_EP = 8


def draw_routes(key, part):
    nblocks = TOKENS // TOK_DEV
    rank = jnp.arange(nblocks, dtype=jnp.int32)
    jitter = jax.random.randint(jax.random.fold_in(key, 11), (nblocks,), 0, 3, dtype=jnp.int32)
    offset = rank * 6 // nblocks + jitter
    places = jnp.arange(TOK_DEV, dtype=jnp.int32)
    first = offset[:, None] + places[None, :] // CAP
    second = offset[:, None] + (places[None, :] + TOK_DEV) // CAP
    paired = jnp.stack([first, second], axis=2) % EXPERTS
    scores = jax.random.randint(jax.random.fold_in(key, 12), (nblocks, TOK_DEV), 0, 1 << 20, dtype=jnp.int32) * TOK_DEV + places[None, :]
    order = jnp.argsort(scores, axis=1, stable=True).astype(jnp.int32)
    paired = jnp.take_along_axis(paired, order[:, :, None], axis=1)
    flipped = jax.random.randint(jax.random.fold_in(key, 13), (nblocks, TOK_DEV, 1), 0, 2, dtype=jnp.int32)
    paired = jnp.where(flipped == 1, paired[:, :, ::-1], paired)
    return paired.reshape(TOKENS, 2).astype(jnp.int32)


def shard_levels(key, shape, pieces, least, high):
    def one(axis_at, parts):
        draws = jax.random.uniform(jax.random.fold_in(jax.random.fold_in(key, 6), axis_at), (parts,), jnp.float32, least / len(pieces), high / len(pieces))
        return jnp.repeat(jnp.exp(draws), shape[axis_at] // parts).reshape((-1,) + (1,) * (len(shape) - axis_at - 1))

    level = one(*pieces[0])
    for cut in pieces[1:]:
        level = level * one(*cut)
    return level


def bell_draw(key, dims, scale, bound, pieces=(), held_as=jnp.bfloat16):
    result = scale * jax.random.normal(key, dims, jnp.float32)
    if pieces:
        result = result * shard_levels(key, dims, pieces, -0.22, 0.18)
    return jnp.clip(result, -bound, bound).astype(held_as)


def setup_inputs(seed: int = 0) -> dict:
    splits = jax.random.split(jax.random.key(seed), 8)
    tokens = bell_draw(splits[0], (TOKENS, D), 1.0, 6.0, ((0, 32),))
    cotangent = bell_draw(splits[1], (TOKENS, D), 0.5, 4.0, ((0, 32),))
    routes = draw_routes(jax.random.fold_in(splits[7], 71), 0)
    logits = bell_draw(splits[3], (TOKENS, EXPERTS), 2.0, 8.0, ((0, 32),), jnp.float32)
    w_gate = bell_draw(splits[4], (D, EXP_WIN * FF), D ** -0.5, 0.125, ((0, 4), (1, 8)))
    w_up = bell_draw(splits[5], (D, EXP_WIN * FF), D ** -0.5, 0.125, ((0, 4), (1, 8)))
    w_down = bell_draw(splits[6], (EXP_WIN * FF, D), FF ** -0.5, 0.0625, ((0, 8), (1, 4)))
    return dict(tokens=tokens, cotangent=cotangent, routes=routes, logits=logits, w_gate=w_gate, w_up=w_up, w_down=w_down)


def routing(routes, logits):
    experts_all = logits.shape[-1]
    picked = (routes[:, :, None] == jnp.arange(experts_all, dtype=jnp.int32)[None, None, :]).astype(jnp.float32)
    chosen = jnp.sum(picked * logits[:, None, :], axis=2)
    combine = jax.nn.softmax(chosen, axis=1)
    window = picked[:, :, :EXP_WIN]
    member = jnp.sum(window, axis=1)
    scaled = jnp.sum(window * combine[:, :, None], axis=1)
    member_int = member.astype(jnp.int32)
    slot_ids = jnp.cumsum(member_int, axis=0) - member_int
    places = jnp.arange(CAP, dtype=jnp.int32)
    select = member[:, :, None] * (slot_ids[:, :, None] == places[None, None, :]).astype(jnp.float32)
    select = jnp.transpose(select, (1, 2, 0))
    slot_weight = jnp.einsum('xct,tx->xc', select, scaled)
    return select, slot_weight


def dispatch(select, slot_weight, tokens, cotangent):
    sent_tokens = jnp.einsum('xct,td->xcd', select, tokens.astype(jnp.float32)).astype(jnp.bfloat16)
    moved = jnp.einsum('xct,td->xcd', select, cotangent.astype(jnp.float32))
    sent_grads = (moved * slot_weight[:, :, None]).astype(jnp.bfloat16)
    return sent_tokens, sent_grads


def aux_gradient(routes, logits, total_counts):
    frac = total_counts.astype(jnp.float32) / jnp.sum(total_counts.astype(jnp.float32))
    probs = jax.nn.softmax(logits, axis=1)
    target = logits.shape[1] * frac
    return probs * (target[None, :] - jnp.sum(probs * target[None, :], axis=1, keepdims=True))


def expert_pass(rows_x, rows_dy, gate_w, up_w, down_w, blocks):
    gate_pre = jnp.dot(rows_x, gate_w, preferred_element_type=jnp.float32)
    up_pre = jnp.dot(rows_x, up_w, preferred_element_type=jnp.float32)
    sigma = jax.nn.sigmoid(gate_pre)
    active = gate_pre * sigma
    hidden = (active * up_pre).astype(jnp.bfloat16)
    hidden_grad = jnp.dot(rows_dy, down_w.T, preferred_element_type=jnp.float32)
    nrows = rows_x.shape[0]
    block_width = gate_w.shape[1] // blocks
    dots = jnp.sum((hidden.astype(jnp.float32) * hidden_grad).reshape(nrows, blocks, block_width), axis=2).astype(jnp.bfloat16)
    dots = jnp.sum(lax.optimization_barrier(dots).astype(jnp.float32), axis=1)
    up_grad = (hidden_grad * active).astype(jnp.bfloat16)
    gate_grad = (hidden_grad * up_pre * sigma * (1.0 + gate_pre * (1.0 - sigma))).astype(jnp.bfloat16)
    width_model = gate_w.shape[0]
    partial_value = jnp.einsum('rsf,dsf->srd', gate_grad.astype(jnp.float32).reshape(nrows, blocks, block_width),
                         gate_w.astype(jnp.float32).reshape(width_model, blocks, block_width))
    partial_value = partial_value + jnp.einsum('rsf,dsf->srd', up_grad.astype(jnp.float32).reshape(nrows, blocks, block_width),
                                   up_w.astype(jnp.float32).reshape(width_model, blocks, block_width))
    partial_value = lax.optimization_barrier(partial_value.astype(jnp.bfloat16))
    slot_grad = jnp.sum(partial_value.astype(jnp.float32), axis=0)
    grad_g = jnp.dot(rows_x.T, gate_grad, preferred_element_type=jnp.float32).astype(jnp.bfloat16)
    grad_u = jnp.dot(rows_x.T, up_grad, preferred_element_type=jnp.float32).astype(jnp.bfloat16)
    grad_d = jnp.dot(hidden.T, rows_dy, preferred_element_type=jnp.float32).astype(jnp.bfloat16)
    return slot_grad, dots, grad_g, grad_u, grad_d


def reference(tokens, cotangent, routes, logits, w_gate, w_up, w_down):
    blocks = N_EP // EXP_WIN
    tok = tokens.reshape(N_FSDP * N_EP, TOK_DEV, D)
    cot = cotangent.reshape(N_FSDP * N_EP, TOK_DEV, D)
    rts = routes.reshape(N_FSDP * N_EP, TOK_DEV, 2)
    lgt = logits.reshape(N_FSDP * N_EP, TOK_DEV, EXPERTS)
    select, slot_weight = jax.vmap(routing)(rts, lgt)
    sent_tokens, sent_grads = jax.vmap(dispatch)(select, slot_weight, tok, cot)
    sent_tokens = sent_tokens.reshape(N_FSDP, N_EP, EXP_WIN, CAP, D)
    sent_grads = sent_grads.reshape(N_FSDP, N_EP, EXP_WIN, CAP, D)

    def group_step(carry, blocks_in):
        acc_gate, acc_up, acc_down = carry
        group_x, group_dy = blocks_in
        grads_out = []
        dots_out = []
        for expert in range(EXP_WIN):
            low = expert * FF
            rows_x = group_x[:, expert].reshape(N_EP * CAP, D)
            rows_dy = group_dy[:, expert].reshape(N_EP * CAP, D)
            slot_grad, dots, grad_g, grad_u, grad_d = expert_pass(
                rows_x, rows_dy, w_gate[:, low:low + FF], w_up[:, low:low + FF], w_down[low:low + FF, :], blocks)
            acc_gate = acc_gate.at[:, low:low + FF].add(grad_g.astype(jnp.float32))
            acc_up = acc_up.at[:, low:low + FF].add(grad_u.astype(jnp.float32))
            acc_down = acc_down.at[low:low + FF, :].add(grad_d.astype(jnp.float32))
            grads_out.append(slot_grad.reshape(N_EP, CAP, D))
            dots_out.append(dots.reshape(N_EP, CAP))
        return (acc_gate, acc_up, acc_down), (jnp.stack(grads_out, axis=1), jnp.stack(dots_out, axis=1))

    start = (jnp.zeros((D, EXP_WIN * FF), jnp.float32), jnp.zeros((D, EXP_WIN * FF), jnp.float32),
             jnp.zeros((EXP_WIN * FF, D), jnp.float32))
    (acc_gate, acc_up, acc_down), (slot_grads, slot_dots) = lax.scan(group_step, start, (sent_tokens, sent_grads))
    slot_grads = slot_grads.reshape(N_FSDP * N_EP, EXP_WIN, CAP, D)
    slot_dots = slot_dots.reshape(N_FSDP * N_EP, EXP_WIN, CAP)
    grad_tokens = jnp.einsum('nxct,nxcd->ntd', select, slot_grads).reshape(TOKENS, D).astype(jnp.bfloat16)
    route_dot = jnp.einsum('nxct,nxc->ntx', select, slot_dots).reshape(TOKENS, EXP_WIN)
    total_counts = jnp.sum((routes[:, :, None] == jnp.arange(EXPERTS, dtype=jnp.int32)[None, None, :]).astype(jnp.int32), axis=(0, 1))
    aux_grad = aux_gradient(routes, logits, total_counts)
    return (grad_tokens, route_dot, aux_grad, acc_gate.astype(jnp.bfloat16), acc_up.astype(jnp.bfloat16),
            acc_down.astype(jnp.bfloat16))
```

```python
import functools

import jax
import jax.numpy as jnp
from jax import lax
from jax.experimental import pallas as pl
from jax.experimental.pallas import tpu as pltpu
from jax.sharding import PartitionSpec as P

EXP_WIN = 2
CAP = 3
PAD = 8
CORES = 2
CHUNKS = 4
GROUPS = 2
PIECES = 4
LAST = (((1,), (1,)), ((), ()))
FIRST = (((0,), (0,)), ((), ()))
F32 = jnp.float32
BF16 = jnp.bfloat16
MESH = pl.DeviceIdType.MESH


def iota(shape, axis):
    return lax.broadcasted_iota(jnp.int32, shape, axis)


def kernel(
    n_fsdp, n_ep, chunks,
    tok_ref, cot_ref, routes_ref, logits_ref, wg_hbm, wu_hbm, wd_hbm,
    gt_ref, rd_ref, aux_ref, og, ou, od,
    wg, wu, wd,
    send1, recv1, rows_x, rows_dy,
    own_a, send_a, recv_a, send_b, recv_b, acts, recv_c, dx, dots, send2, recv2,
    w_sem, d_send, d_recv, a_send, a_recv, b_send, b_recv, c_send, c_recv, r_send, r_recv,
):
    n_dev = n_fsdp * n_ep
    n_x = n_fsdp // CORES
    blocks = n_ep // EXP_WIN
    f, e = lax.axis_index("fsdp"), lax.axis_index("ep")
    me = f * n_ep + e
    x, core = f // CORES, lax.rem(f, CORES)
    partner = x * CORES + (1 - core)
    depth, width = wg.shape
    half = width // CORES
    w = half // chunks
    ring = n_ep // GROUPS
    size = n_fsdp * ring
    span_rows = size * CAP
    place = f * ring + e // GROUPS

    def peer(t, i):
        return i // ring, lax.rem(i, ring) * GROUPS + lax.rem(e + t, GROUPS)

    barrier = pltpu.get_barrier_semaphore()

    def greet(j, _):
        d = lax.rem(me + j, n_dev)
        pl.semaphore_signal(barrier, inc=1, device_id=(d // n_ep, lax.rem(d, n_ep)), device_id_type=MESH)
        return 0

    lax.fori_loop(1, n_dev, greet, 0)
    loads = [
        pltpu.make_async_copy(s, t, w_sem.at[i])
        for i, (s, t) in enumerate(((wg_hbm, wg), (wu_hbm, wu), (wd_hbm, wd)))
    ]
    for c in loads:
        c.start()

    routes = routes_ref[...]
    logits = logits_ref[...]
    n_tok, n_exp = logits.shape
    ti, tj = iota((n_tok, n_tok), 0), iota((n_tok, n_tok), 1)
    r0, r1 = (
        jnp.sum(jnp.where(ti == tj, routes[k : k + 1, :], 0), axis=1, keepdims=True) for k in range(2)
    )
    experts = iota((n_tok, n_exp), 1)
    c0 = jnp.sum(jnp.where(experts == r0, logits, 0.0), axis=1, keepdims=True)
    c1 = jnp.sum(jnp.where(experts == r1, logits, 0.0), axis=1, keepdims=True)
    top = jnp.maximum(c0, c1)
    e0, e1 = jnp.exp(c0 - top), jnp.exp(c1 - top)
    p0, p1 = e0 / (e0 + e1), e1 / (e0 + e1)
    ci = iota((PAD, n_tok), 0)
    lanes = iota((n_tok, depth), 1)
    counts = jnp.sum(
        jnp.where(lanes == r0, 1.0, 0.0) + jnp.where(lanes == r1, 1.0, 0.0), axis=0, keepdims=True
    )
    tok = tok_ref[...]
    cot = cot_ref[...].astype(F32)
    member_col, slot_col, member_row, slot_line = [], [], [], []
    row_id = iota((PAD, depth), 0)
    for k in range(EXP_WIN):
        m0, m1 = jnp.where(r0 == k, 1.0, 0.0), jnp.where(r1 == k, 1.0, 0.0)
        col = m0 + m1
        weight = m0 * p0 + m1 * p1
        row = jnp.sum(jnp.where(ti == tj, col, 0.0), axis=0, keepdims=True)
        slot_row = jnp.sum(jnp.where(ti < tj, col, 0.0), axis=0, keepdims=True)
        slot_col.append(jnp.sum(jnp.where(tj < ti, row, 0.0), axis=1, keepdims=True))
        member_col.append(col)
        member_row.append(row)
        slot_line.append(slot_row)
        cf = ci.astype(F32)
        sel_a = jnp.where((cf == slot_row) & (ci < CAP), row, 0.0).astype(BF16)
        sel_b = jnp.where((cf - CAP == slot_row) & (ci < 2 * CAP), row, 0.0).astype(BF16)
        wcot = (cot * weight).astype(BF16)
        sent = jnp.dot(sel_a, tok, preferred_element_type=F32)
        sent = sent + jnp.dot(sel_b, wcot, preferred_element_type=F32)
        for g in range(n_fsdp):
            part = sent[:, g * depth : (g + 1) * depth]
            send1[k, g] = jnp.where(row_id == 2 * CAP, counts, part).astype(BF16)

    pl.semaphore_wait(barrier, n_dev - 1)

    recv1[place] = send1[e // blocks, f]
    for t in range(GROUPS):
        back_t = (GROUPS - t) % GROUPS

        def push(j, _, t=t, back_t=back_t):
            df, de = peer(t, lax.rem(place + j, size))
            pltpu.make_async_remote_copy(
                src_ref=send1.at[de // blocks, df], dst_ref=recv1.at[back_t * size + place],
                send_sem=d_send, recv_sem=d_recv.at[back_t], device_id=(df, de), device_id_type=MESH,
            ).start()
            return 0

        lax.fori_loop(1 if t == 0 else 0, size, push, 0)

    grp = min(16, size)
    si, sj = iota((grp * CAP, grp * PAD), 0), iota((grp * CAP, grp * PAD), 1)
    base = (si // CAP) * PAD + lax.rem(si, CAP)
    pick_x = jnp.where(sj == base, 1.0, 0.0).astype(BF16)
    pick_dy = jnp.where(sj == base + CAP, 1.0, 0.0).astype(BF16)
    pick_c = jnp.where(
        lax.rem(iota((8, grp * PAD), 1), PAD) == 2 * CAP, 1.0, 0.0
    ).astype(BF16)

    def prepare(t, total):
        landed = recv1.at[pl.ds(t * size, size - 1 if t == 0 else size)]
        pltpu.make_async_copy(landed, landed, d_recv.at[t]).wait()
        for g in range(t * size // grp, (t + 1) * size // grp):
            came = recv1[g * grp : (g + 1) * grp].reshape(grp * PAD, depth)
            span = pl.ds(g * grp * CAP, grp * CAP)
            rows_x[span] = jnp.dot(pick_x, came, preferred_element_type=F32).astype(BF16)
            rows_dy[span] = jnp.dot(pick_dy, came, preferred_element_type=F32).astype(BF16)
            total = total + jnp.dot(pick_c, came, preferred_element_type=F32)
        return total

    def copy_a(k):
        return pltpu.make_async_remote_copy(
            src_ref=send_a.at[k], dst_ref=recv_a.at[k], send_sem=a_send.at[k], recv_sem=a_recv.at[k],
            device_id=(partner, e), device_id_type=MESH,
        )

    def copy_b(k, j):
        to = lax.rem(x + j, n_x) * CORES + core
        return pltpu.make_async_remote_copy(
            src_ref=send_b.at[k], dst_ref=recv_b.at[k, j - 1], send_sem=b_send.at[k, j - 1],
            recv_sem=b_recv.at[k, j - 1], device_id=(to, e), device_id_type=MESH,
        )

    def copy_c(k):
        return pltpu.make_async_remote_copy(
            src_ref=acts.at[k], dst_ref=recv_c.at[k], send_sem=c_send.at[k], recv_sem=c_recv.at[k],
            device_id=(partner, e), device_id_type=MESH,
        )

    def columns(h, k):
        return pl.ds(pl.multiple_of(h * half + k * w, w), w)

    def group(u):
        return pl.ds(u // chunks * span_rows, span_rows)

    def partials(h, u):
        cols = columns(h, u % chunks)
        xs, dys = rows_x[group(u)], rows_dy[group(u)]
        yield jnp.dot(xs, wg[:, cols], preferred_element_type=F32)
        yield jnp.dot(xs, wu[:, cols], preferred_element_type=F32)
        yield lax.dot_general(dys, wd[cols, :], LAST, preferred_element_type=F32)

    def stage1(k):
        for i, v in enumerate(partials(1 - core, k)):
            send_a[k, i] = v.astype(BF16)
        copy_a(k).start()
        for i, v in enumerate(partials(core, k)):
            own_a[k, i] = v

    def stage2(k):
        copy_a(k).wait_recv()
        v = own_a[k] + recv_a[k].astype(F32)
        own_a[k] = v
        send_b[k] = v.astype(BF16)
        for j in range(1, n_x):
            copy_b(k, j).start()

    def stage3(k):
        for j in range(1, n_x):
            copy_b(k, j).wait_recv()
        pre = []
        for i in range(3):
            v = own_a[k, i]
            for j in range(n_x - 1):
                v = v + recv_b[k, j, i].astype(F32)
            pre.append(v)
        gate_pre, up_pre, hidden_grad = pre
        sigma = jax.nn.sigmoid(gate_pre)
        active = gate_pre * sigma
        hidden = (active * up_pre).astype(BF16)
        dot = jnp.sum(hidden.astype(F32) * hidden_grad, axis=1, keepdims=True)
        dots[group(k)] = dot if k % chunks == 0 else dots[group(k)] + dot
        acts[k, 0] = (hidden_grad * up_pre * sigma * (1.0 + gate_pre * (1.0 - sigma))).astype(BF16)
        acts[k, 1] = (hidden_grad * active).astype(BF16)
        acts[k, 2] = hidden
        copy_c(k).start()

    def grads(h, k, source):
        cols = columns(h, k % chunks)
        part = lax.dot_general(source[k, 0], wg[:, cols], LAST, preferred_element_type=F32)
        return part + lax.dot_general(source[k, 1], wu[:, cols], LAST, preferred_element_type=F32)

    def weights(c):
        for h, source in ((core, acts), (1 - core, recv_c)):
            cols = columns(h, c)
            ga, ua, hid = (
                jnp.concatenate([source[t * chunks + c, i] for t in range(GROUPS)], axis=0) for i in range(3)
            )
            xs, dys = rows_x[...], rows_dy[...]
            og[:, cols] = lax.dot_general(xs, ga, FIRST, preferred_element_type=F32).astype(BF16)
            ou[:, cols] = lax.dot_general(xs, ua, FIRST, preferred_element_type=F32).astype(BF16)
            od[cols, :] = lax.dot_general(hid, dys, FIRST, preferred_element_type=F32).astype(BF16)

    def stage4(k):
        part = grads(core, k, acts)
        copy_c(k).wait_recv()
        part = part + grads(1 - core, k, recv_c)
        dx[group(k)] = part if k % chunks == 0 else dx[group(k)] + part

    for c in loads:
        c.wait()
    total = jnp.zeros((8, depth), F32)
    for t in range(GROUPS):
        total = prepare(t, total)
        for k in range(t * chunks, (t + 1) * chunks):
            stage1(k)
            if k > 0:
                stage2(k - 1)
    stage2(GROUPS * chunks - 1)

    count = total[0:1, 0:n_exp]
    target = n_exp * (count / jnp.sum(count, axis=1, keepdims=True))
    raised = jnp.exp(logits - jnp.max(logits, axis=1, keepdims=True))
    probs = raised / jnp.sum(raised, axis=1, keepdims=True)
    aux_ref[...] = probs * (target - jnp.sum(probs * target, axis=1, keepdims=True))

    bi, bj = iota((grp * PAD, grp * CAP), 0), iota((grp * PAD, grp * CAP), 1)
    base = (bj // CAP) * PAD + lax.rem(bj, CAP)
    put_x = jnp.where(bi == base, 1.0, 0.0).astype(BF16)
    put_dot = jnp.where(bi == base + CAP, 1.0, 0.0).astype(BF16)
    once = jnp.where(x == 0, 1.0, 0.0)

    def give_back(t):
        for g in range(t * size // grp, (t + 1) * size // grp):
            span = pl.ds(g * grp * CAP, grp * CAP)
            mine = jnp.broadcast_to(dots[span] * once, (grp * CAP, depth)).astype(BF16)
            back = jnp.dot(put_x, dx[span].astype(BF16), preferred_element_type=F32)
            back = back + jnp.dot(put_dot, mine, preferred_element_type=F32)
            send2[g * grp : (g + 1) * grp] = back.astype(BF16).reshape(grp, PAD, depth)

        def give(j, _):
            i = lax.rem(place + j, size)
            pltpu.make_async_remote_copy(
                src_ref=send2.at[t * size + i], dst_ref=recv2.at[me], send_sem=r_send, recv_sem=r_recv,
                device_id=peer(t, i), device_id_type=MESH,
            ).start()
            return 0

        lax.fori_loop(1 if t == 0 else 0, size, give, 0)
        if t == 0:
            recv2[me] = send2[place]

    for k in range(GROUPS * chunks):
        stage3(k)
        if k > 0:
            stage4(k - 1)
            if k % chunks == 0:
                give_back(k // chunks - 1)
    stage4(GROUPS * chunks - 1)
    give_back(GROUPS - 1)
    for c in range(chunks):
        weights(c)
    everyone = recv1.at[pl.ds(0, n_dev - 1)]
    everyone2 = recv2.at[pl.ds(0, n_dev - 1)]
    pltpu.make_async_copy(everyone2, everyone2, r_recv).wait()

    route = [jnp.zeros((1, 1), F32) for _ in range(EXP_WIN * CAP)]
    for g in range(n_fsdp):
        grad = jnp.zeros((n_tok, depth), F32)
        for k in range(EXP_WIN):
            acc = recv2[g * n_ep + k * blocks].astype(F32)
            for b in range(1, blocks):
                acc = acc + recv2[g * n_ep + k * blocks + b].astype(F32)
            for c in range(CAP):
                pick = jnp.where(slot_col[k] == c, member_col[k], 0.0)
                grad = grad + pick * acc[c : c + 1, :]
                route[k * CAP + c] = route[k * CAP + c] + acc[CAP + c : CAP + c + 1, 0:1]
        gt_ref[:, g * depth : (g + 1) * depth] = grad.astype(BF16)
    which = iota((EXP_WIN, n_tok), 0)
    out = jnp.zeros((EXP_WIN, n_tok), F32)
    for k in range(EXP_WIN):
        for c in range(CAP):
            pick = jnp.where(slot_line[k] == c, member_row[k], 0.0)
            out = out + jnp.where(which == k, pick * route[k * CAP + c], 0.0)
    rd_ref[...] = out

    pltpu.make_async_copy(everyone, everyone, d_send).wait()
    pltpu.make_async_copy(everyone2, everyone2, r_send).wait()
    for k in range(GROUPS * chunks):
        copy_a(k).wait_send()
        copy_c(k).wait_send()
        for j in range(1, n_x):
            copy_b(k, j).wait_send()


def put_kernel(n, *refs):
    sources, targets, sem = refs[:n], refs[n : 2 * n], refs[2 * n]
    copies = []
    for s, t in zip(sources, targets):
        rows = s.shape[0]
        pieces = PIECES if rows % (16 * PIECES) == 0 else 1
        for p in range(pieces):
            span = pl.ds(p * (rows // pieces), rows // pieces)
            copies.append(pltpu.make_async_copy(s.at[span], t.at[span], sem.at[len(copies)]))
    for c in copies:
        c.start()
    for c in copies:
        c.wait()


def body(n_fsdp, n_ep, tokens, cotangent, routes, logits, w_gate, w_up, w_down):
    n_tok, model = tokens.shape
    depth, width = w_gate.shape
    n_dev = n_fsdp * n_ep
    n_x = n_fsdp // CORES
    rows = n_dev * CAP
    half = width // CORES
    chunks = max(1, min(CHUNKS, half // 128))
    w = half // chunks
    items, part = GROUPS * chunks, rows // GROUPS
    vmem = pl.BlockSpec(memory_space=pltpu.VMEM)
    hbm = pl.BlockSpec(memory_space=pl.ANY)
    dma = pltpu.SemaphoreType.DMA
    made = (
        ((n_tok, model), BF16),
        ((EXP_WIN, n_tok), F32),
        (logits.shape, F32),
        (w_gate.shape, BF16),
        (w_up.shape, BF16),
        (w_down.shape, BF16),
    )
    held = pl.pallas_call(
        functools.partial(kernel, n_fsdp, n_ep, chunks),
        out_shape=tuple(pltpu.VMEM(d, t) for d, t in made),
        in_specs=[vmem] * 4 + [hbm] * 3,
        out_specs=[vmem] * 6,
        scratch_shapes=[
            pltpu.VMEM(w_gate.shape, BF16),
            pltpu.VMEM(w_up.shape, BF16),
            pltpu.VMEM(w_down.shape, BF16),
            pltpu.VMEM((EXP_WIN, n_fsdp, PAD, depth), BF16),
            pltpu.VMEM((n_dev, PAD, depth), BF16),
            pltpu.VMEM((rows, depth), BF16),
            pltpu.VMEM((rows, depth), BF16),
            pltpu.VMEM((items, 3, part, w), F32),
            pltpu.VMEM((items, 3, part, w), BF16),
            pltpu.VMEM((items, 3, part, w), BF16),
            pltpu.VMEM((items, 3, part, w), BF16),
            pltpu.VMEM((items, n_x - 1, 3, part, w), BF16),
            pltpu.VMEM((items, 3, part, w), BF16),
            pltpu.VMEM((items, 3, part, w), BF16),
            pltpu.VMEM((rows, depth), F32),
            pltpu.VMEM((rows, 1), F32),
            pltpu.VMEM((n_dev, PAD, depth), BF16),
            pltpu.VMEM((n_dev, PAD, depth), BF16),
            dma((3,)),
            dma,
            dma((GROUPS,)),
            dma((items,)),
            dma((items,)),
            dma((items, n_x - 1)),
            dma((items, n_x - 1)),
            dma((items,)),
            dma((items,)),
            dma,
            dma,
        ],
        compiler_params=pltpu.CompilerParams(
            collective_id=0, has_side_effects=True, vmem_limit_bytes=54 * 1024 * 1024
        ),
    )(tokens, cotangent, jnp.transpose(routes), logits, w_gate, w_up, w_down)
    out = pl.pallas_call(
        functools.partial(put_kernel, len(made)),
        out_shape=tuple(jax.ShapeDtypeStruct(d, t) for d, t in made),
        in_specs=[vmem] * len(made),
        out_specs=[hbm] * len(made),
        scratch_shapes=[dma((PIECES * len(made),))],
        compiler_params=pltpu.CompilerParams(vmem_limit_bytes=1024 * 1024),
    )(*held)
    return (out[0], jnp.transpose(out[1])) + tuple(out[2:])


def solution(mesh):
    in_specs = (
        P(("fsdp", "ep"), None),
        P(("fsdp", "ep"), None),
        P(("fsdp", "ep"), None),
        P(("fsdp", "ep"), None),
        P("fsdp", "ep"),
        P("fsdp", "ep"),
        P("ep", "fsdp"),
    )
    out_specs = (
        P(("fsdp", "ep"), None),
        P(("fsdp", "ep"), None),
        P(("fsdp", "ep"), None),
        P("fsdp", "ep"),
        P("fsdp", "ep"),
        P("ep", "fsdp"),
    )
    step = functools.partial(body, mesh.shape["fsdp"], mesh.shape["ep"])
    return jax.shard_map(step, mesh=mesh, in_specs=in_specs, out_specs=out_specs, check_vma=False)
```

```python
import functools

import jax
import jax.numpy as jnp
from jax import lax
from jax.experimental import pallas as pl
from jax.experimental.pallas import tpu as pltpu
from jax.sharding import PartitionSpec as P

EXP_WIN = 2
CAP = 3
PAD = 8
CORES = 2
CHUNKS = 4
GROUPS = EXP_WIN
LANES = 128
PIECES = 4
LAST = (((1,), (1,)), ((), ()))
FIRST = (((0,), (0,)), ((), ()))
F32 = jnp.float32
BF16 = jnp.bfloat16
MESH = pl.DeviceIdType.MESH


def iota(shape, axis):
    return lax.broadcasted_iota(jnp.int32, shape, axis)


def kernel(
    n_fsdp, n_ep, chunks, sub,
    tok_hbm, cot_hbm, routes_hbm, logits_hbm, wg_hbm, wu_hbm, wd_hbm,
    gt_ref, rd_ref, aux_ref, og, ou, od,
    tok_ref, cot_ref, routes_ref, logits_ref, wg, wu, wd,
    send1, recv1, rows_x, rows_dy,
    own_a, send_a, recv_a, send_b, recv_b, acts, recv_c, dx, dots, send2, recv2, put, final,
    i_sem, w_sem, d_send, d_recv, s_send, s_recv, a_send, a_recv, b_send, b_recv, c_send, c_recv, r_send, r_recv,
):
    n_dev = n_fsdp * n_ep
    n_x = n_fsdp // CORES
    blocks = n_ep // EXP_WIN
    f, e = lax.axis_index("fsdp"), lax.axis_index("ep")
    me = f * n_ep + e
    x, core = f // CORES, lax.rem(f, CORES)
    partner = x * CORES + (1 - core)
    half_of, block = e // blocks, lax.rem(e, blocks)
    other = 1 - half_of
    depth, width = wg.shape
    half = width // CORES
    w = half // chunks
    size = n_fsdp * blocks
    span_rows = size * CAP
    place = block * n_fsdp + f
    pieces = depth // LANES

    def member(t, i):
        return lax.rem(i, n_fsdp), (half_of if t == 0 else other) * blocks + i // n_fsdp

    barrier = pltpu.get_barrier_semaphore()

    def greet(j, _):
        pl.semaphore_signal(barrier, inc=1, device_id=member(0, lax.rem(place + j, size)), device_id_type=MESH)
        return 0

    def greet_other(j, _):
        pl.semaphore_signal(barrier, inc=1, device_id=(j, other * blocks + block), device_id_type=MESH)
        return 0

    lax.fori_loop(0, n_fsdp, greet_other, 0)
    lax.fori_loop(1, size, greet, 0)
    smalls = [
        pltpu.make_async_copy(s, t, i_sem.at[i])
        for i, (s, t) in enumerate(
            ((routes_hbm, routes_ref), (logits_hbm, logits_ref), (tok_hbm, tok_ref), (cot_hbm, cot_ref))
        )
    ]
    loads = [
        pltpu.make_async_copy(s, t, w_sem.at[i])
        for i, (s, t) in enumerate(((wg_hbm, wg), (wu_hbm, wu), (wd_hbm, wd)))
    ]
    for c in smalls + loads:
        c.start()
    for c in smalls:
        c.wait()

    routes = routes_ref[...]
    logits = logits_ref[...]
    n_tok, n_exp = logits.shape
    ti, tj = iota((n_tok, n_tok), 0), iota((n_tok, n_tok), 1)
    r0, r1 = (
        jnp.sum(jnp.where(ti == tj, routes[k : k + 1, :], 0), axis=1, keepdims=True) for k in range(2)
    )
    experts = iota((n_tok, n_exp), 1)
    c0 = jnp.sum(jnp.where(experts == r0, logits, 0.0), axis=1, keepdims=True)
    c1 = jnp.sum(jnp.where(experts == r1, logits, 0.0), axis=1, keepdims=True)
    top = jnp.maximum(c0, c1)
    e0, e1 = jnp.exp(c0 - top), jnp.exp(c1 - top)
    p0, p1 = e0 / (e0 + e1), e1 / (e0 + e1)
    ci = iota((PAD, n_tok), 0)
    tok = tok_ref[...]
    cot = cot_ref[...].astype(F32)
    member_col, slot_col = [], []
    for k in range(EXP_WIN):
        m0, m1 = jnp.where(r0 == k, 1.0, 0.0), jnp.where(r1 == k, 1.0, 0.0)
        col = m0 + m1
        weight = m0 * p0 + m1 * p1
        row = jnp.sum(jnp.where(ti == tj, col, 0.0), axis=0, keepdims=True)
        slot_row = jnp.sum(jnp.where(ti < tj, col, 0.0), axis=0, keepdims=True)
        slot_col.append(jnp.sum(jnp.where(tj < ti, row, 0.0), axis=1, keepdims=True))
        member_col.append(col)
        cf = ci.astype(F32)
        sel_a = jnp.where((cf == slot_row) & (ci < CAP), row, 0.0).astype(BF16)
        sel_b = jnp.where((cf - CAP == slot_row) & (ci < 2 * CAP), row, 0.0).astype(BF16)
        wcot = (cot * weight).astype(BF16)
        sent = jnp.dot(sel_a, tok, preferred_element_type=F32)
        sent = sent + jnp.dot(sel_b, wcot, preferred_element_type=F32)
        for g in range(n_fsdp):
            send1[k, g] = sent[:, g * depth : (g + 1) * depth].astype(BF16)

    pl.semaphore_wait(barrier, size - 1 + n_fsdp)

    def push(j, _):
        i = lax.rem(place + j, size)
        pltpu.make_async_remote_copy(
            src_ref=send1.at[half_of, lax.rem(i, n_fsdp)], dst_ref=recv1.at[place],
            send_sem=d_send, recv_sem=d_recv.at[0], device_id=member(0, i), device_id_type=MESH,
        ).start()
        return 0

    def push_other(j, _):
        g = lax.rem(f + j, n_fsdp)
        pltpu.make_async_remote_copy(
            src_ref=send1.at[other, g], dst_ref=recv1.at[size + place],
            send_sem=d_send, recv_sem=d_recv.at[1], device_id=(g, other * blocks + block), device_id_type=MESH,
        ).start()
        return 0

    lax.fori_loop(1, size, push, 0)
    lax.fori_loop(0, n_fsdp, push_other, 0)
    recv1[place] = send1[half_of, f]

    shared = recv1.at[pl.ds(size + block * n_fsdp, n_fsdp)]

    def share(j):
        return pltpu.make_async_remote_copy(
            src_ref=shared, dst_ref=shared, send_sem=s_send, recv_sem=s_recv,
            device_id=(f, half_of * blocks + lax.rem(block + j, blocks)), device_id_type=MESH,
        )

    def relay():
        pltpu.make_async_copy(shared, shared, d_recv.at[1]).wait()

        def one(j, _):
            share(j).start()
            return 0

        lax.fori_loop(1, blocks, one, 0)

    grp = min(16, size)
    lanes = iota((n_tok, LANES), 1)
    counts = jnp.sum(
        jnp.where(lanes == r0, 1.0, 0.0) + jnp.where(lanes == r1, 1.0, 0.0), axis=0, keepdims=True
    )
    raised = jnp.exp(logits - jnp.max(logits, axis=1, keepdims=True))
    probs = raised / jnp.sum(raised, axis=1, keepdims=True)
    put_shape = (grp * sub, (pieces + 1) * grp * CAP)
    pi, pj = iota(put_shape, 0), iota(put_shape, 1)
    pr = lax.rem(pj, grp * CAP)
    put[...] = jnp.where(
        (pi // sub == pr // CAP) & (lax.rem(pi, sub) == pj // (grp * CAP) * CAP + lax.rem(pr, CAP)), 1.0, 0.0
    ).astype(BF16)
    reach = n_ep * sub
    fj = iota((n_tok, reach), 1)
    fk, fs = fj // (blocks * sub), lax.rem(fj, sub).astype(F32)
    picks = []
    for q in range(pieces):
        row = jnp.zeros((n_tok, reach), F32)
        for k in range(EXP_WIN):
            row = row + jnp.where((fk == k) & (fs == slot_col[k] + q * CAP), member_col[k], 0.0)
        picks.append(row)
    for k in range(EXP_WIN):
        picks.append(jnp.where((fk == k) & (fs == slot_col[k] + pieces * CAP), member_col[k], 0.0))
    picks.append(jnp.where(fs == (pieces + 1) * CAP, 1.0, 0.0))
    final[...] = jnp.concatenate(picks, axis=0).astype(BF16)

    si, sj = iota((grp * CAP, grp * PAD), 0), iota((grp * CAP, grp * PAD), 1)
    base = (si // CAP) * PAD + lax.rem(si, CAP)
    pick_x = jnp.where(sj == base, 1.0, 0.0).astype(BF16)
    pick_dy = jnp.where(sj == base + CAP, 1.0, 0.0).astype(BF16)

    def prepare(t):
        if t == 0:
            landed = recv1.at[pl.ds(0, size - 1)]
            pltpu.make_async_copy(landed, landed, d_recv.at[0]).wait()
        elif blocks > 1:
            landed = recv1.at[pl.ds(0, (blocks - 1) * n_fsdp)]
            pltpu.make_async_copy(landed, landed, s_recv).wait()
        for g in range(t * size // grp, (t + 1) * size // grp):
            came = recv1[g * grp : (g + 1) * grp].reshape(grp * PAD, depth)
            span = pl.ds(g * grp * CAP, grp * CAP)
            rows_x[span] = jnp.dot(pick_x, came, preferred_element_type=F32).astype(BF16)
            rows_dy[span] = jnp.dot(pick_dy, came, preferred_element_type=F32).astype(BF16)

    def copy_a(k):
        return pltpu.make_async_remote_copy(
            src_ref=send_a.at[k], dst_ref=recv_a.at[k], send_sem=a_send.at[k], recv_sem=a_recv.at[k],
            device_id=(partner, e), device_id_type=MESH,
        )

    def copy_b(k, j):
        to = lax.rem(x + j, n_x) * CORES + core
        return pltpu.make_async_remote_copy(
            src_ref=send_b.at[k], dst_ref=recv_b.at[k, j - 1], send_sem=b_send.at[k, j - 1],
            recv_sem=b_recv.at[k, j - 1], device_id=(to, e), device_id_type=MESH,
        )

    def copy_c(k):
        return pltpu.make_async_remote_copy(
            src_ref=acts.at[k], dst_ref=recv_c.at[k], send_sem=c_send.at[k], recv_sem=c_recv.at[k],
            device_id=(partner, e), device_id_type=MESH,
        )

    def columns(h, k):
        return pl.ds(pl.multiple_of(h * half + k * w, w), w)

    def group(u):
        return pl.ds(u // chunks * span_rows, span_rows)

    def partials(h, u):
        cols = columns(h, u % chunks)
        xs, dys = rows_x[group(u)], rows_dy[group(u)]
        yield jnp.dot(xs, wg[:, cols], preferred_element_type=F32)
        yield jnp.dot(xs, wu[:, cols], preferred_element_type=F32)
        yield lax.dot_general(dys, wd[cols, :], LAST, preferred_element_type=F32)

    def stage1(k):
        for i, v in enumerate(partials(1 - core, k)):
            send_a[k, i] = v.astype(BF16)
        copy_a(k).start()
        for i, v in enumerate(partials(core, k)):
            own_a[k, i] = v

    def stage2(k):
        copy_a(k).wait_recv()
        v = own_a[k] + recv_a[k].astype(F32)
        own_a[k] = v
        send_b[k] = v.astype(BF16)
        for j in range(1, n_x):
            copy_b(k, j).start()

    def stage3(k):
        for j in range(1, n_x):
            copy_b(k, j).wait_recv()
        pre = []
        for i in range(3):
            v = own_a[k, i]
            for j in range(n_x - 1):
                v = v + recv_b[k, j, i].astype(F32)
            pre.append(v)
        gate_pre, up_pre, hidden_grad = pre
        sigma = jax.nn.sigmoid(gate_pre)
        active = gate_pre * sigma
        hidden = (active * up_pre).astype(BF16)
        dot = jnp.sum(hidden.astype(F32) * hidden_grad, axis=1, keepdims=True)
        dots[group(k)] = dot if k % chunks == 0 else dots[group(k)] + dot
        acts[k, 0] = (hidden_grad * up_pre * sigma * (1.0 + gate_pre * (1.0 - sigma))).astype(BF16)
        acts[k, 1] = (hidden_grad * active).astype(BF16)
        acts[k, 2] = hidden
        copy_c(k).start()

    def grads(h, k, source):
        cols = columns(h, k % chunks)
        part = lax.dot_general(source[k, 0], wg[:, cols], LAST, preferred_element_type=F32)
        return part + lax.dot_general(source[k, 1], wu[:, cols], LAST, preferred_element_type=F32)

    def weights(c):
        for h, source in ((core, acts), (1 - core, recv_c)):
            cols = columns(h, c)
            ga, ua, hid = (
                jnp.concatenate([source[t * chunks + c, i] for t in range(GROUPS)], axis=0) for i in range(3)
            )
            xs, dys = rows_x[...], rows_dy[...]
            og[:, cols] = lax.dot_general(xs, ga, FIRST, preferred_element_type=F32).astype(BF16)
            ou[:, cols] = lax.dot_general(xs, ua, FIRST, preferred_element_type=F32).astype(BF16)
            od[cols, :] = lax.dot_general(hid, dys, FIRST, preferred_element_type=F32).astype(BF16)

    def stage4(k):
        part = grads(core, k, acts)
        copy_c(k).wait_recv()
        part = part + grads(1 - core, k, recv_c)
        dx[group(k)] = part if k % chunks == 0 else dx[group(k)] + part

    for c in loads:
        c.wait()
    for t in range(GROUPS):
        prepare(t)
        for k in range(t * chunks, (t + 1) * chunks):
            stage1(k)
            if k > 0:
                stage2(k - 1)
            if k == 1:
                relay()
        if chunks == 1 and t == 0:
            relay()
    stage2(GROUPS * chunks - 1)

    once = jnp.where(x == 0, 1.0, 0.0)
    mark = lax.rem(iota((grp * sub, LANES), 0), sub) == (pieces + 1) * CAP

    def give_back(t):
        for g in range(t * size // grp, (t + 1) * size // grp):
            span = pl.ds(g * grp * CAP, grp * CAP)
            grads = dx[span].astype(BF16)
            mine = jnp.broadcast_to(dots[span] * once, (grp * CAP, LANES)).astype(BF16)
            stack = [grads[:, q * LANES : (q + 1) * LANES] for q in range(pieces)] + [mine]
            back = jnp.dot(put[...], jnp.concatenate(stack, axis=0), preferred_element_type=F32)
            back = jnp.where(mark, counts, back).astype(BF16)
            send2[g * grp : (g + 1) * grp] = back.reshape(grp, sub, LANES)

        def give(j, _):
            i = lax.rem(place + j, size)
            pltpu.make_async_remote_copy(
                src_ref=send2.at[t * size + i], dst_ref=recv2.at[me], send_sem=r_send, recv_sem=r_recv,
                device_id=member(t, i), device_id_type=MESH,
            ).start()
            return 0

        lax.fori_loop(1 if t == 0 else 0, size, give, 0)
        if t == 0:
            recv2[me] = send2[place]

    for k in range(GROUPS * chunks):
        stage3(k)
        if k > 0:
            stage4(k - 1)
            if k % chunks == 0:
                give_back(k // chunks - 1)
    stage4(GROUPS * chunks - 1)
    give_back(GROUPS - 1)
    for c in range(chunks):
        weights(c)
    everyone2 = recv2.at[pl.ds(0, n_dev - 1)]
    pltpu.make_async_copy(everyone2, everyone2, r_recv).wait()

    rest = jnp.zeros(((EXP_WIN + 1) * n_tok, LANES), F32)
    for g in range(n_fsdp):
        came = recv2[g * n_ep : (g + 1) * n_ep].reshape(reach, LANES)
        made = jnp.dot(final[...], came, preferred_element_type=F32)
        for q in range(pieces):
            at = g * depth + q * LANES
            gt_ref[:, at : at + LANES] = made[q * n_tok : (q + 1) * n_tok].astype(BF16)
        rest = rest + made[pieces * n_tok :]
    for k in range(EXP_WIN):
        col = rest[k * n_tok : (k + 1) * n_tok, 0:n_tok]
        rd_ref[k : k + 1, :] = jnp.sum(jnp.where(ti == tj, col, 0.0), axis=0, keepdims=True)
    count = rest[EXP_WIN * n_tok : EXP_WIN * n_tok + 1, 0:n_exp]
    target = n_exp * (count / jnp.sum(count, axis=1, keepdims=True))
    aux_ref[...] = probs * (target - jnp.sum(probs * target, axis=1, keepdims=True))

    everyone = recv1.at[pl.ds(0, size - 1 + n_fsdp)]
    pltpu.make_async_copy(everyone, everyone, d_send).wait()
    if blocks > 1:
        passed = recv1.at[pl.ds(0, (blocks - 1) * n_fsdp)]
        pltpu.make_async_copy(passed, passed, s_send).wait()
    pltpu.make_async_copy(everyone2, everyone2, r_send).wait()
    for k in range(GROUPS * chunks):
        copy_a(k).wait_send()
        copy_c(k).wait_send()
        for j in range(1, n_x):
            copy_b(k, j).wait_send()


def put_kernel(n, *refs):
    sources, targets, sem = refs[:n], refs[n : 2 * n], refs[2 * n]
    copies = []
    for s, t in zip(sources, targets):
        rows = s.shape[0]
        pieces = PIECES if rows % (16 * PIECES) == 0 else 1
        for p in range(pieces):
            span = pl.ds(p * (rows // pieces), rows // pieces)
            copies.append(pltpu.make_async_copy(s.at[span], t.at[span], sem.at[len(copies)]))
    for c in copies:
        c.start()
    for c in copies:
        c.wait()


def body(n_fsdp, n_ep, tokens, cotangent, routes, logits, w_gate, w_up, w_down):
    n_tok, model = tokens.shape
    depth, width = w_gate.shape
    n_dev = n_fsdp * n_ep
    n_x = n_fsdp // CORES
    rows = n_dev * CAP
    half = width // CORES
    chunks = max(1, min(CHUNKS, half // 128))
    w = half // chunks
    items, part = GROUPS * chunks, rows // GROUPS
    pieces = depth // LANES
    sub = -(-((pieces + 1) * CAP + 1) // 8) * 8
    grp = min(16, n_dev // EXP_WIN)
    vmem = pl.BlockSpec(memory_space=pltpu.VMEM)
    hbm = pl.BlockSpec(memory_space=pl.ANY)
    dma = pltpu.SemaphoreType.DMA
    made = (
        ((n_tok, model), BF16),
        ((EXP_WIN, n_tok), F32),
        (logits.shape, F32),
        (w_gate.shape, BF16),
        (w_up.shape, BF16),
        (w_down.shape, BF16),
    )
    held = pl.pallas_call(
        functools.partial(kernel, n_fsdp, n_ep, chunks, sub),
        out_shape=tuple(pltpu.VMEM(d, t) for d, t in made),
        in_specs=[hbm] * 7,
        out_specs=[vmem] * 6,
        scratch_shapes=[
            pltpu.VMEM(tokens.shape, BF16),
            pltpu.VMEM(cotangent.shape, BF16),
            pltpu.VMEM(routes.shape[::-1], routes.dtype),
            pltpu.VMEM(logits.shape, F32),
            pltpu.VMEM(w_gate.shape, BF16),
            pltpu.VMEM(w_up.shape, BF16),
            pltpu.VMEM(w_down.shape, BF16),
            pltpu.VMEM((EXP_WIN, n_fsdp, PAD, depth), BF16),
            pltpu.VMEM((n_dev, PAD, depth), BF16),
            pltpu.VMEM((rows, depth), BF16),
            pltpu.VMEM((rows, depth), BF16),
            pltpu.VMEM((items, 3, part, w), F32),
            pltpu.VMEM((items, 3, part, w), BF16),
            pltpu.VMEM((items, 3, part, w), BF16),
            pltpu.VMEM((items, 3, part, w), BF16),
            pltpu.VMEM((items, n_x - 1, 3, part, w), BF16),
            pltpu.VMEM((items, 3, part, w), BF16),
            pltpu.VMEM((items, 3, part, w), BF16),
            pltpu.VMEM((rows, depth), F32),
            pltpu.VMEM((rows, 1), F32),
            pltpu.VMEM((n_dev, sub, LANES), BF16),
            pltpu.VMEM((n_dev, sub, LANES), BF16),
            pltpu.VMEM((grp * sub, (pieces + 1) * grp * CAP), BF16),
            pltpu.VMEM(((pieces + EXP_WIN + 1) * n_tok, n_ep * sub), BF16),
            dma((4,)),
            dma((3,)),
            dma,
            dma((GROUPS,)),
            dma,
            dma,
            dma((items,)),
            dma((items,)),
            dma((items, n_x - 1)),
            dma((items, n_x - 1)),
            dma((items,)),
            dma((items,)),
            dma,
            dma,
        ],
        compiler_params=pltpu.CompilerParams(
            collective_id=0, has_side_effects=True, vmem_limit_bytes=54 * 1024 * 1024
        ),
    )(tokens, cotangent, jnp.transpose(routes), logits, w_gate, w_up, w_down)
    out = pl.pallas_call(
        functools.partial(put_kernel, len(made)),
        out_shape=tuple(jax.ShapeDtypeStruct(d, t) for d, t in made),
        in_specs=[vmem] * len(made),
        out_specs=[hbm] * len(made),
        scratch_shapes=[dma((PIECES * len(made),))],
        compiler_params=pltpu.CompilerParams(vmem_limit_bytes=1024 * 1024),
    )(*held)
    return (out[0], jnp.transpose(out[1])) + tuple(out[2:])


def solution(mesh):
    in_specs = (
        P(("fsdp", "ep"), None),
        P(("fsdp", "ep"), None),
        P(("fsdp", "ep"), None),
        P(("fsdp", "ep"), None),
        P("fsdp", "ep"),
        P("fsdp", "ep"),
        P("ep", "fsdp"),
    )
    out_specs = (
        P(("fsdp", "ep"), None),
        P(("fsdp", "ep"), None),
        P(("fsdp", "ep"), None),
        P("fsdp", "ep"),
        P("fsdp", "ep"),
        P("ep", "fsdp"),
    )
    step = functools.partial(body, mesh.shape["fsdp"], mesh.shape["ep"])
    return jax.shard_map(step, mesh=mesh, in_specs=in_specs, out_specs=out_specs, check_vma=False)
```

```python
import functools

import jax
import jax.numpy as jnp
from jax import lax
from jax.experimental import pallas as pl
from jax.experimental.pallas import tpu as pltpu
from jax.sharding import PartitionSpec as P

EXP_WIN = 2
CAP = 3
CORES = 2
CHUNKS = 4
GROUPS = EXP_WIN
LANES = 128
PIECES = 4
LAST = (((1,), (1,)), ((), ()))
FIRST = (((0,), (0,)), ((), ()))
F32 = jnp.float32
BF16 = jnp.bfloat16
MESH = pl.DeviceIdType.MESH


def iota(shape, axis):
    return lax.broadcasted_iota(jnp.int32, shape, axis)


def kernel(
    n_fsdp, n_ep, chunks, sub, pack,
    tok_hbm, cot_hbm, routes_hbm, logits_hbm, wg_hbm, wu_hbm, wd_hbm,
    gt_ref, rd_ref, aux_ref, og, ou, od,
    tok_ref, cot_ref, routes_ref, logits_ref, wg, wu, wd,
    send1, recv1, rows_x, rows_dy,
    own_a, send_a, recv_a, send_b, recv_b, acts, recv_c, dx, dots, send2, recv2, put, pick, final,
    i_sem, w_sem, d_send, d_recv, s_send, s_recv, a_send, a_recv, b_send, b_recv, c_send, c_recv, r_send, r_recv,
):
    n_dev = n_fsdp * n_ep
    n_x = n_fsdp // CORES
    blocks = n_ep // EXP_WIN
    f, e = lax.axis_index("fsdp"), lax.axis_index("ep")
    me = f * n_ep + e
    x, core = f // CORES, lax.rem(f, CORES)
    partner = x * CORES + (1 - core)
    half_of, block = e // blocks, lax.rem(e, blocks)
    other = 1 - half_of
    depth, width = wg.shape
    half = width // CORES
    w = half // chunks
    size = n_fsdp * blocks
    span_rows = size * CAP
    place = block * n_fsdp + f
    pieces = depth // LANES

    columns_f = [lax.rem(f + j, n_fsdp) for j in range(n_fsdp)]

    def visit(act, own):
        def row(j, first=0):
            b = lax.rem(block + j, blocks)
            for g in columns_f[first:]:
                act(g, b)

        if blocks <= 4:
            for j in range(1, blocks):
                row(j)
        else:
            lax.fori_loop(1, blocks, lambda j, _: (row(j), 0)[1], 0)
        row(0, 0 if own else 1)

    smalls = [
        pltpu.make_async_copy(s, t, i_sem.at[i])
        for i, (s, t) in enumerate(
            ((routes_hbm, routes_ref), (logits_hbm, logits_ref), (tok_hbm, tok_ref), (cot_hbm, cot_ref))
        )
    ]
    for c in smalls:
        c.start()

    barrier = pltpu.get_barrier_semaphore()

    def greet(g, at):
        pl.semaphore_signal(barrier, inc=1, device_id=(g, at), device_id_type=MESH)

    for g in columns_f:
        greet(g, other * blocks + block)
    visit(lambda g, b: greet(g, half_of * blocks + b), False)
    loads = [
        pltpu.make_async_copy(s, t, w_sem.at[i])
        for i, (s, t) in enumerate(((wg_hbm, wg), (wu_hbm, wu), (wd_hbm, wd)))
    ]
    for c in smalls:
        c.wait()
    for c in loads:
        c.start()

    routes = routes_ref[...]
    logits = logits_ref[...]
    n_tok, n_exp = logits.shape
    ti, tj = iota((n_tok, n_tok), 0), iota((n_tok, n_tok), 1)
    r0, r1 = (
        jnp.sum(jnp.where(ti == tj, routes[k : k + 1, :], 0), axis=1, keepdims=True) for k in range(2)
    )
    experts = iota((n_tok, n_exp), 1)
    c0 = jnp.sum(jnp.where(experts == r0, logits, 0.0), axis=1, keepdims=True)
    c1 = jnp.sum(jnp.where(experts == r1, logits, 0.0), axis=1, keepdims=True)
    top = jnp.maximum(c0, c1)
    e0, e1 = jnp.exp(c0 - top), jnp.exp(c1 - top)
    p0, p1 = e0 / (e0 + e1), e1 / (e0 + e1)
    spread = pieces * n_tok
    wi, wj = iota((pack, 2 * spread), 0), iota((pack, 2 * spread), 1)
    wq, wp = wi // (2 * CAP), lax.rem(wi, 2 * CAP)
    want = (wq == lax.rem(wj, spread) // n_tok) & (wp // CAP == wj // spread)
    slot_of = lax.rem(wp, CAP).astype(F32)
    ui, uj = iota((n_tok, 2 * spread), 0), lax.rem(iota((n_tok, 2 * spread), 1), n_tok)

    def cut(v):
        return jnp.concatenate(
            [
                jnp.concatenate(
                    [v[:, g * depth + q * LANES : g * depth + (q + 1) * LANES] for g in range(n_fsdp)], axis=1
                )
                for q in range(pieces)
            ],
            axis=0,
        )

    tok = cut(tok_ref[...].astype(F32))
    cot = cut(cot_ref[...].astype(F32))
    member_col, slot_col = [], []
    for k in range(EXP_WIN):
        m0, m1 = jnp.where(r0 == k, 1.0, 0.0), jnp.where(r1 == k, 1.0, 0.0)
        col = m0 + m1
        weight = m0 * p0 + m1 * p1
        mine = jnp.sum(jnp.where(ui == uj, col, 0.0), axis=0, keepdims=True)
        slot = jnp.sum(jnp.where(ui < uj, col, 0.0), axis=0, keepdims=True)
        row = jnp.sum(jnp.where(ti == tj, col, 0.0), axis=0, keepdims=True)
        slot_col.append(jnp.sum(jnp.where(tj < ti, row, 0.0), axis=1, keepdims=True))
        member_col.append(col)
        sel = jnp.where(want & (slot_of == slot), mine, 0.0).astype(BF16)
        weighted = cot * jnp.concatenate([weight] * pieces, axis=0)
        both = jnp.concatenate([tok, weighted], axis=0).astype(BF16)
        sent = jnp.dot(sel, both, preferred_element_type=F32).astype(BF16)
        for g in range(n_fsdp):
            send1[k, g] = sent[:, g * LANES : (g + 1) * LANES]

    pl.semaphore_wait(barrier, size - 1 + n_fsdp)

    def push(g, b):
        pltpu.make_async_remote_copy(
            src_ref=send1.at[half_of, g], dst_ref=recv1.at[place], send_sem=d_send, recv_sem=d_recv.at[0],
            device_id=(g, half_of * blocks + b), device_id_type=MESH,
        ).start()

    visit(push, False)
    for g in columns_f:
        pltpu.make_async_remote_copy(
            src_ref=send1.at[other, g], dst_ref=recv1.at[size + place],
            send_sem=d_send, recv_sem=d_recv.at[1], device_id=(g, other * blocks + block), device_id_type=MESH,
        ).start()
    recv1[place] = send1[half_of, f]

    shared = recv1.at[pl.ds(size + block * n_fsdp, n_fsdp)]

    def share(j):
        return pltpu.make_async_remote_copy(
            src_ref=shared, dst_ref=shared, send_sem=s_send, recv_sem=s_recv,
            device_id=(f, half_of * blocks + lax.rem(block + j, blocks)), device_id_type=MESH,
        )

    def relay():
        pltpu.make_async_copy(shared, shared, d_recv.at[1]).wait()

        def one(j, _):
            share(j).start()
            return 0

        lax.fori_loop(1, blocks, one, 0)

    grp = min(16, size)
    lanes = iota((n_tok, LANES), 1)
    counts = jnp.sum(
        jnp.where(lanes == r0, 1.0, 0.0) + jnp.where(lanes == r1, 1.0, 0.0), axis=0, keepdims=True
    )
    raised = jnp.exp(logits - jnp.max(logits, axis=1, keepdims=True))
    probs = raised / jnp.sum(raised, axis=1, keepdims=True)
    put_shape = (grp * sub, (pieces + 1) * grp * CAP)
    pi, pj = iota(put_shape, 0), iota(put_shape, 1)
    pr = lax.rem(pj, grp * CAP)
    put[...] = jnp.where(
        (pi // sub == pr // CAP) & (lax.rem(pi, sub) == pj // (grp * CAP) * CAP + lax.rem(pr, CAP)), 1.0, 0.0
    ).astype(BF16)
    reach = n_ep * sub
    fj = iota((n_tok, reach), 1)
    fk, fs = fj // (blocks * sub), lax.rem(fj, sub).astype(F32)
    picks = []
    for q in range(pieces):
        row = jnp.zeros((n_tok, reach), F32)
        for k in range(EXP_WIN):
            row = row + jnp.where((fk == k) & (fs == slot_col[k] + q * CAP), member_col[k], 0.0)
        picks.append(row)
    for k in range(EXP_WIN):
        picks.append(jnp.where((fk == k) & (fs == slot_col[k] + pieces * CAP), member_col[k], 0.0))
    picks.append(jnp.where(fs == (pieces + 1) * CAP, 1.0, 0.0))
    final[...] = jnp.concatenate(picks, axis=0).astype(BF16)

    rows = grp * CAP
    pick_shape = (2 * pieces * rows, grp * pack)
    si, sj = iota(pick_shape, 0), iota(pick_shape, 1)
    sr, sb = lax.rem(si, rows), si // rows
    pick[...] = jnp.where(
        sj == sr // CAP * pack + lax.rem(sb, pieces) * 2 * CAP + sb // pieces * CAP + lax.rem(sr, CAP), 1.0, 0.0
    ).astype(BF16)

    def prepare(t):
        if t == 0:
            landed = recv1.at[pl.ds(0, size - 1)]
            pltpu.make_async_copy(landed, landed, d_recv.at[0]).wait()
        elif blocks > 1:
            landed = recv1.at[pl.ds(0, (blocks - 1) * n_fsdp)]
            pltpu.make_async_copy(landed, landed, s_recv).wait()
        for g in range(t * size // grp, (t + 1) * size // grp):
            came = recv1[g * grp : (g + 1) * grp].reshape(grp * pack, LANES)
            found = jnp.dot(pick[...], came, preferred_element_type=F32).astype(BF16)
            span = pl.ds(g * rows, rows)
            for q in range(pieces):
                at = slice(q * LANES, (q + 1) * LANES)
                rows_x[span, at] = found[q * rows : (q + 1) * rows]
                rows_dy[span, at] = found[(pieces + q) * rows : (pieces + q + 1) * rows]

    def copy_a(k):
        return pltpu.make_async_remote_copy(
            src_ref=send_a.at[k], dst_ref=recv_a.at[k], send_sem=a_send.at[k], recv_sem=a_recv.at[k],
            device_id=(partner, e), device_id_type=MESH,
        )

    def copy_b(k, j):
        to = lax.rem(x + j, n_x) * CORES + core
        return pltpu.make_async_remote_copy(
            src_ref=send_b.at[k], dst_ref=recv_b.at[k, j - 1], send_sem=b_send.at[k, j - 1],
            recv_sem=b_recv.at[k, j - 1], device_id=(to, e), device_id_type=MESH,
        )

    def copy_c(k):
        return pltpu.make_async_remote_copy(
            src_ref=acts.at[k], dst_ref=recv_c.at[k], send_sem=c_send.at[k], recv_sem=c_recv.at[k],
            device_id=(partner, e), device_id_type=MESH,
        )

    def columns(h, k):
        return pl.ds(pl.multiple_of(h * half + k * w, w), w)

    def group(u):
        return pl.ds(u // chunks * span_rows, span_rows)

    def partials(h, u):
        cols = columns(h, u % chunks)
        xs, dys = rows_x[group(u)], rows_dy[group(u)]
        yield jnp.dot(xs, wg[:, cols], preferred_element_type=F32)
        yield jnp.dot(xs, wu[:, cols], preferred_element_type=F32)
        yield lax.dot_general(dys, wd[cols, :], LAST, preferred_element_type=F32)

    def stage1(k):
        for i, v in enumerate(partials(1 - core, k)):
            send_a[k, i] = v.astype(BF16)
        copy_a(k).start()
        for i, v in enumerate(partials(core, k)):
            own_a[k, i] = v

    def stage2(k):
        copy_a(k).wait_recv()
        v = own_a[k] + recv_a[k].astype(F32)
        own_a[k] = v
        send_b[k] = v.astype(BF16)
        for j in range(1, n_x):
            copy_b(k, j).start()

    def stage3(k):
        for j in range(1, n_x):
            copy_b(k, j).wait_recv()
        pre = []
        for i in range(3):
            v = own_a[k, i]
            for j in range(n_x - 1):
                v = v + recv_b[k, j, i].astype(F32)
            pre.append(v)
        gate_pre, up_pre, hidden_grad = pre
        sigma = jax.nn.sigmoid(gate_pre)
        active = gate_pre * sigma
        hidden = (active * up_pre).astype(BF16)
        dot = jnp.sum(hidden.astype(F32) * hidden_grad, axis=1, keepdims=True)
        dots[group(k)] = dot if k % chunks == 0 else dots[group(k)] + dot
        acts[k, 0] = (hidden_grad * up_pre * sigma * (1.0 + gate_pre * (1.0 - sigma))).astype(BF16)
        acts[k, 1] = (hidden_grad * active).astype(BF16)
        acts[k, 2] = hidden
        copy_c(k).start()

    def grads(h, k, source):
        cols = columns(h, k % chunks)
        part = lax.dot_general(source[k, 0], wg[:, cols], LAST, preferred_element_type=F32)
        return part + lax.dot_general(source[k, 1], wu[:, cols], LAST, preferred_element_type=F32)

    def weights(c):
        for h, source in ((core, acts), (1 - core, recv_c)):
            cols = columns(h, c)
            ga, ua, hid = (
                jnp.concatenate([source[t * chunks + c, i] for t in range(GROUPS)], axis=0) for i in range(3)
            )
            xs, dys = rows_x[...], rows_dy[...]
            og[:, cols] = lax.dot_general(xs, ga, FIRST, preferred_element_type=F32).astype(BF16)
            ou[:, cols] = lax.dot_general(xs, ua, FIRST, preferred_element_type=F32).astype(BF16)
            od[cols, :] = lax.dot_general(hid, dys, FIRST, preferred_element_type=F32).astype(BF16)

    def stage4(k):
        part = grads(core, k, acts)
        copy_c(k).wait_recv()
        part = part + grads(1 - core, k, recv_c)
        dx[group(k)] = part if k % chunks == 0 else dx[group(k)] + part

    for c in loads:
        c.wait()
    lead = max(1, chunks - 1)
    order = [*range(lead), *range(chunks, 2 * chunks), *range(lead, chunks)]
    prepare(0)
    for i, k in enumerate(order):
        if i == lead:
            stage2(order[i - 1])
            prepare(1)
        stage1(k)
        if i > 0 and i != lead:
            stage2(order[i - 1])
        if i == 0:
            relay()
    stage2(order[-1])

    once = jnp.where(x == 0, 1.0, 0.0)
    mark = lax.rem(iota((grp * sub, LANES), 0), sub) == (pieces + 1) * CAP

    def give_back(t):
        for g in range(t * size // grp, (t + 1) * size // grp):
            span = pl.ds(g * grp * CAP, grp * CAP)
            grads = dx[span].astype(BF16)
            mine = jnp.broadcast_to(dots[span] * once, (grp * CAP, LANES)).astype(BF16)
            stack = [grads[:, q * LANES : (q + 1) * LANES] for q in range(pieces)] + [mine]
            back = jnp.dot(put[...], jnp.concatenate(stack, axis=0), preferred_element_type=F32)
            back = jnp.where(mark, counts, back).astype(BF16)
            send2[g * grp : (g + 1) * grp] = back.reshape(grp, sub, LANES)

        def give(g, b):
            pltpu.make_async_remote_copy(
                src_ref=send2.at[t * size + b * n_fsdp + g], dst_ref=recv2.at[me], send_sem=r_send, recv_sem=r_recv,
                device_id=(g, (other if t else half_of) * blocks + b), device_id_type=MESH,
            ).start()

        visit(give, t > 0)
        if t == 0:
            recv2[me] = send2[place]

    for i, k in enumerate(order):
        stage3(k)
        if i > 0 and order[i - 1] != 2 * chunks - 1:
            stage4(order[i - 1])
        if k == 2 * chunks - 1:
            stage4(k)
            give_back(1)
    if order[-1] != 2 * chunks - 1:
        stage4(order[-1])
    give_back(0)
    for c in range(chunks):
        weights(c)
    everyone2 = recv2.at[pl.ds(0, n_dev - 1)]
    everyone = recv1.at[pl.ds(0, size - 1 + n_fsdp)]
    pltpu.make_async_copy(everyone, everyone, d_send).wait()
    if blocks > 1:
        passed = recv1.at[pl.ds(0, (blocks - 1) * n_fsdp)]
        pltpu.make_async_copy(passed, passed, s_send).wait()
    pltpu.make_async_copy(everyone2, everyone2, r_send).wait()
    for k in range(GROUPS * chunks):
        copy_a(k).wait_send()
        copy_c(k).wait_send()
        for j in range(1, n_x):
            copy_b(k, j).wait_send()
    pltpu.make_async_copy(everyone2, everyone2, r_recv).wait()

    rest = jnp.zeros(((EXP_WIN + 1) * n_tok, LANES), F32)
    for g in range(n_fsdp):
        came = recv2[g * n_ep : (g + 1) * n_ep].reshape(reach, LANES)
        made = jnp.dot(final[...], came, preferred_element_type=F32)
        for q in range(pieces):
            at = g * depth + q * LANES
            gt_ref[:, at : at + LANES] = made[q * n_tok : (q + 1) * n_tok].astype(BF16)
        rest = rest + made[pieces * n_tok :]
    for k in range(EXP_WIN):
        col = rest[k * n_tok : (k + 1) * n_tok, 0:n_tok]
        rd_ref[k : k + 1, :] = jnp.sum(jnp.where(ti == tj, col, 0.0), axis=0, keepdims=True)
    count = rest[EXP_WIN * n_tok : EXP_WIN * n_tok + 1, 0:n_exp]
    target = n_exp * (count / (2 * n_tok * n_dev))
    aux_ref[...] = probs * (target - jnp.sum(probs * target, axis=1, keepdims=True))


def put_kernel(n, *refs):
    sources, targets, sem = refs[:n], refs[n : 2 * n], refs[2 * n]
    copies = []
    for s, t in zip(sources, targets):
        rows = s.shape[0]
        pieces = PIECES if rows % (16 * PIECES) == 0 else 1
        for p in range(pieces):
            span = pl.ds(p * (rows // pieces), rows // pieces)
            copies.append(pltpu.make_async_copy(s.at[span], t.at[span], sem.at[len(copies)]))
    for c in copies:
        c.start()
    for c in copies:
        c.wait()


def body(n_fsdp, n_ep, tokens, cotangent, routes, logits, w_gate, w_up, w_down):
    n_tok, model = tokens.shape
    depth, width = w_gate.shape
    n_dev = n_fsdp * n_ep
    n_x = n_fsdp // CORES
    rows = n_dev * CAP
    half = width // CORES
    chunks = max(1, min(CHUNKS, half // 128))
    w = half // chunks
    items, part = GROUPS * chunks, rows // GROUPS
    pieces = depth // LANES
    sub = -(-((pieces + 1) * CAP + 1) // 8) * 8
    pack = -(-2 * CAP * pieces // 8) * 8
    grp = min(16, n_dev // EXP_WIN)
    vmem = pl.BlockSpec(memory_space=pltpu.VMEM)
    hbm = pl.BlockSpec(memory_space=pl.ANY)
    dma = pltpu.SemaphoreType.DMA
    made = (
        ((n_tok, model), BF16),
        ((EXP_WIN, n_tok), F32),
        (logits.shape, F32),
        (w_gate.shape, BF16),
        (w_up.shape, BF16),
        (w_down.shape, BF16),
    )
    held = pl.pallas_call(
        functools.partial(kernel, n_fsdp, n_ep, chunks, sub, pack),
        out_shape=tuple(pltpu.VMEM(d, t) for d, t in made),
        in_specs=[hbm] * 7,
        out_specs=[vmem] * 6,
        scratch_shapes=[
            pltpu.VMEM(tokens.shape, BF16),
            pltpu.VMEM(cotangent.shape, BF16),
            pltpu.VMEM(routes.shape[::-1], routes.dtype),
            pltpu.VMEM(logits.shape, F32),
            pltpu.VMEM(w_gate.shape, BF16),
            pltpu.VMEM(w_up.shape, BF16),
            pltpu.VMEM(w_down.shape, BF16),
            pltpu.VMEM((EXP_WIN, n_fsdp, pack, LANES), BF16),
            pltpu.VMEM((n_dev, pack, LANES), BF16),
            pltpu.VMEM((rows, depth), BF16),
            pltpu.VMEM((rows, depth), BF16),
            pltpu.VMEM((items, 3, part, w), F32),
            pltpu.VMEM((items, 3, part, w), BF16),
            pltpu.VMEM((items, 3, part, w), BF16),
            pltpu.VMEM((items, 3, part, w), BF16),
            pltpu.VMEM((items, n_x - 1, 3, part, w), BF16),
            pltpu.VMEM((items, 3, part, w), BF16),
            pltpu.VMEM((items, 3, part, w), BF16),
            pltpu.VMEM((rows, depth), F32),
            pltpu.VMEM((rows, 1), F32),
            pltpu.VMEM((n_dev, sub, LANES), BF16),
            pltpu.VMEM((n_dev, sub, LANES), BF16),
            pltpu.VMEM((grp * sub, (pieces + 1) * grp * CAP), BF16),
            pltpu.VMEM((2 * pieces * grp * CAP, grp * pack), BF16),
            pltpu.VMEM(((pieces + EXP_WIN + 1) * n_tok, n_ep * sub), BF16),
            dma((4,)),
            dma((3,)),
            dma,
            dma((GROUPS,)),
            dma,
            dma,
            dma((items,)),
            dma((items,)),
            dma((items, n_x - 1)),
            dma((items, n_x - 1)),
            dma((items,)),
            dma((items,)),
            dma,
            dma,
        ],
        compiler_params=pltpu.CompilerParams(
            collective_id=0, has_side_effects=True, vmem_limit_bytes=54 * 1024 * 1024
        ),
    )(tokens, cotangent, jnp.transpose(routes), logits, w_gate, w_up, w_down)
    out = pl.pallas_call(
        functools.partial(put_kernel, len(made)),
        out_shape=tuple(jax.ShapeDtypeStruct(d, t) for d, t in made),
        in_specs=[vmem] * len(made),
        out_specs=[hbm] * len(made),
        scratch_shapes=[dma((PIECES * len(made),))],
        compiler_params=pltpu.CompilerParams(vmem_limit_bytes=1024 * 1024),
    )(*held)
    return (out[0], jnp.transpose(out[1])) + tuple(out[2:])


def solution(mesh):
    in_specs = (
        P(("fsdp", "ep"), None),
        P(("fsdp", "ep"), None),
        P(("fsdp", "ep"), None),
        P(("fsdp", "ep"), None),
        P("fsdp", "ep"),
        P("fsdp", "ep"),
        P("ep", "fsdp"),
    )
    out_specs = (
        P(("fsdp", "ep"), None),
        P(("fsdp", "ep"), None),
        P(("fsdp", "ep"), None),
        P("fsdp", "ep"),
        P("fsdp", "ep"),
        P("ep", "fsdp"),
    )
    step = functools.partial(body, mesh.shape["fsdp"], mesh.shape["ep"])
    return jax.shard_map(step, mesh=mesh, in_specs=in_specs, out_specs=out_specs, check_vma=False)
```

```python
import functools

import jax
import jax.numpy as jnp
from jax import lax
from jax.experimental import pallas as pl
from jax.experimental.pallas import tpu as pltpu
from jax.sharding import PartitionSpec as P

EXP_WIN = 2
CAP = 3
CORES = 2
FRONT = (1, 2, 2)
MIDDLE = (1, 2, 2, 2, 1)
BACK = (2, 1)
EARLY = True
GROUPS = EXP_WIN
LANES = 128
PIECES = 8
RING = 4
LAST = (((1,), (1,)), ((), ()))
FIRST = (((0,), (0,)), ((), ()))
F32 = jnp.float32
BF16 = jnp.bfloat16
MESH = pl.DeviceIdType.MESH


def iota(shape, axis):
    return lax.broadcasted_iota(jnp.int32, shape, axis)


def plan(half):
    if half % (8 * LANES):
        return ((0, 0, half), (1, 0, half))
    u = half // 8
    cuts = FRONT + BACK
    items = [(0, u * sum(cuts[:i]), u * c) for i, c in enumerate(cuts)]
    far = [(1, u * sum(MIDDLE[:i]), u * c) for i, c in enumerate(MIDDLE)]
    return (*items[: len(FRONT)], *far, *items[len(FRONT) :])


def kernel(
    n_fsdp, n_ep, order, sub, pack,
    tok_hbm, cot_hbm, routes_hbm, logits_hbm, wg_hbm, wu_hbm, wd_hbm,
    gt_ref, rd_ref, aux_ref, og, ou, od,
    tok_ref, cot_ref, routes_ref, logits_ref, wg, wu, wd,
    send1, recv1, rows_x, rows_dy,
    own_a, send_a, recv_a, send_b, recv_b, acts, recv_c, dx, dots, send2, recv2, put, pick, final,
    i_sem, w_sem, d_send, d_recv, s_send, s_recv, a_send, a_recv, b_send, b_recv, c_send, c_recv, r_send, r_recv,
):
    n_dev = n_fsdp * n_ep
    n_x = n_fsdp // CORES
    blocks = n_ep // EXP_WIN
    f, e = lax.axis_index("fsdp"), lax.axis_index("ep")
    me = f * n_ep + e
    x, core = f // CORES, lax.rem(f, CORES)
    partner = x * CORES + (1 - core)
    half_of, block = e // blocks, lax.rem(e, blocks)
    other = 1 - half_of
    depth, width = wg.shape
    half = width // CORES
    size = n_fsdp * blocks
    span_rows = size * CAP
    place = block * n_fsdp + f
    pieces = depth // LANES

    columns_f = [lax.rem(f + j, n_fsdp) for j in range(n_fsdp)]

    def visit(act, own):
        def row(j, first=0):
            b = lax.rem(block + j, blocks)
            for g in columns_f[first:]:
                act(g, b)

        if blocks <= 4:
            for j in range(1, blocks):
                row(j)
        else:
            lax.fori_loop(1, blocks, lambda j, _: (row(j), 0)[1], 0)
        row(0, 0 if own else 1)

    smalls = [
        pltpu.make_async_copy(s, t, i_sem.at[i])
        for i, (s, t) in enumerate(
            ((routes_hbm, routes_ref), (logits_hbm, logits_ref), (tok_hbm, tok_ref), (cot_hbm, cot_ref))
        )
    ]
    for c in smalls:
        c.start()

    barrier = pltpu.get_barrier_semaphore()

    def greet(g, at):
        pl.semaphore_signal(barrier, inc=1, device_id=(g, at), device_id_type=MESH)

    for g in columns_f:
        greet(g, other * blocks + block)
    visit(lambda g, b: greet(g, half_of * blocks + b), False)
    loads = [
        pltpu.make_async_copy(s, t, w_sem.at[i])
        for i, (s, t) in enumerate(((wg_hbm, wg), (wu_hbm, wu), (wd_hbm, wd)))
    ]
    for c in smalls:
        c.wait()
    for c in loads:
        c.start()

    routes = routes_ref[...]
    logits = logits_ref[...]
    n_tok, n_exp = logits.shape
    ti, tj = iota((n_tok, n_tok), 0), iota((n_tok, n_tok), 1)
    r0, r1 = (
        jnp.sum(jnp.where(ti == tj, routes[k : k + 1, :], 0), axis=1, keepdims=True) for k in range(2)
    )
    experts = iota((n_tok, n_exp), 1)
    c0 = jnp.sum(jnp.where(experts == r0, logits, 0.0), axis=1, keepdims=True)
    c1 = jnp.sum(jnp.where(experts == r1, logits, 0.0), axis=1, keepdims=True)
    top = jnp.maximum(c0, c1)
    e0, e1 = jnp.exp(c0 - top), jnp.exp(c1 - top)
    p0, p1 = e0 / (e0 + e1), e1 / (e0 + e1)
    spread = pieces * n_tok
    wi, wj = iota((pack, 2 * spread), 0), iota((pack, 2 * spread), 1)
    wq, wp = wi // (2 * CAP), lax.rem(wi, 2 * CAP)
    want = (wq == lax.rem(wj, spread) // n_tok) & (wp // CAP == wj // spread)
    slot_of = lax.rem(wp, CAP).astype(F32)
    ui, uj = iota((n_tok, 2 * spread), 0), lax.rem(iota((n_tok, 2 * spread), 1), n_tok)

    def cut(v):
        return jnp.concatenate(
            [
                jnp.concatenate(
                    [v[:, g * depth + q * LANES : g * depth + (q + 1) * LANES] for g in range(n_fsdp)], axis=1
                )
                for q in range(pieces)
            ],
            axis=0,
        )

    tok = cut(tok_ref[...].astype(F32))
    cot = cut(cot_ref[...].astype(F32))
    member_col, slot_col = [], []
    for k in range(EXP_WIN):
        m0, m1 = jnp.where(r0 == k, 1.0, 0.0), jnp.where(r1 == k, 1.0, 0.0)
        col = m0 + m1
        weight = m0 * p0 + m1 * p1
        mine = jnp.sum(jnp.where(ui == uj, col, 0.0), axis=0, keepdims=True)
        slot = jnp.sum(jnp.where(ui < uj, col, 0.0), axis=0, keepdims=True)
        row = jnp.sum(jnp.where(ti == tj, col, 0.0), axis=0, keepdims=True)
        slot_col.append(jnp.sum(jnp.where(tj < ti, row, 0.0), axis=1, keepdims=True))
        member_col.append(col)
        sel = jnp.where(want & (slot_of == slot), mine, 0.0).astype(BF16)
        weighted = cot * jnp.concatenate([weight] * pieces, axis=0)
        both = jnp.concatenate([tok, weighted], axis=0).astype(BF16)
        sent = jnp.dot(sel, both, preferred_element_type=F32).astype(BF16)
        for g in range(n_fsdp):
            send1[k, g] = sent[:, g * LANES : (g + 1) * LANES]

    pl.semaphore_wait(barrier, size - 1 + n_fsdp)

    def push(g, b):
        pltpu.make_async_remote_copy(
            src_ref=send1.at[half_of, g], dst_ref=recv1.at[place], send_sem=d_send, recv_sem=d_recv.at[0],
            device_id=(g, half_of * blocks + b), device_id_type=MESH,
        ).start()

    visit(push, False)
    for g in columns_f:
        pltpu.make_async_remote_copy(
            src_ref=send1.at[other, g], dst_ref=recv1.at[size + place],
            send_sem=d_send, recv_sem=d_recv.at[1], device_id=(g, other * blocks + block), device_id_type=MESH,
        ).start()
    recv1[place] = send1[half_of, f]

    shared = recv1.at[pl.ds(size + block * n_fsdp, n_fsdp)]

    def share(j):
        return pltpu.make_async_remote_copy(
            src_ref=shared, dst_ref=shared, send_sem=s_send, recv_sem=s_recv,
            device_id=(f, half_of * blocks + lax.rem(block + j, blocks)), device_id_type=MESH,
        )

    def relay():
        pltpu.make_async_copy(shared, shared, d_recv.at[1]).wait()

        if blocks <= 4:
            for j in range(1, blocks):
                share(j).start()
        else:
            lax.fori_loop(1, blocks, lambda j, _: (share(j).start(), 0)[1], 0)

    grp = min(16, size)
    lanes = iota((n_tok, LANES), 1)
    counts = jnp.sum(
        jnp.where(lanes == r0, 1.0, 0.0) + jnp.where(lanes == r1, 1.0, 0.0), axis=0, keepdims=True
    )
    raised = jnp.exp(logits - jnp.max(logits, axis=1, keepdims=True))
    probs = raised / jnp.sum(raised, axis=1, keepdims=True)
    put_shape = (grp * sub, (pieces + 1) * grp * CAP)
    pi, pj = iota(put_shape, 0), iota(put_shape, 1)
    pr = lax.rem(pj, grp * CAP)
    put[...] = jnp.where(
        (pi // sub == pr // CAP) & (lax.rem(pi, sub) == pj // (grp * CAP) * CAP + lax.rem(pr, CAP)), 1.0, 0.0
    ).astype(BF16)
    reach = n_ep * sub
    fj = iota((n_tok, reach), 1)
    fk, fs = fj // (blocks * sub), lax.rem(fj, sub).astype(F32)
    picks = []
    for q in range(pieces):
        row = jnp.zeros((n_tok, reach), F32)
        for k in range(EXP_WIN):
            row = row + jnp.where((fk == k) & (fs == slot_col[k] + q * CAP), member_col[k], 0.0)
        picks.append(row)
    for k in range(EXP_WIN):
        picks.append(jnp.where((fk == k) & (fs == slot_col[k] + pieces * CAP), member_col[k], 0.0))
    picks.append(jnp.where(fs == (pieces + 1) * CAP, 1.0, 0.0))
    final[...] = jnp.concatenate(picks, axis=0).astype(BF16)

    rows = grp * CAP
    pick_shape = (2 * pieces * rows, grp * pack)
    si, sj = iota(pick_shape, 0), iota(pick_shape, 1)
    sr, sb = lax.rem(si, rows), si // rows
    pick[...] = jnp.where(
        sj == sr // CAP * pack + lax.rem(sb, pieces) * 2 * CAP + sb // pieces * CAP + lax.rem(sr, CAP), 1.0, 0.0
    ).astype(BF16)

    def prepare(t):
        if t == 0:
            landed = recv1.at[pl.ds(0, size - 1)]
            pltpu.make_async_copy(landed, landed, d_recv.at[0]).wait()
            relay()
        elif blocks > 1:
            landed = recv1.at[pl.ds(0, (blocks - 1) * n_fsdp)]
            pltpu.make_async_copy(landed, landed, s_recv).wait()
        for g in range(t * size // grp, (t + 1) * size // grp):
            came = recv1[g * grp : (g + 1) * grp].reshape(grp * pack, LANES)
            found = jnp.dot(pick[...], came, preferred_element_type=F32).astype(BF16)
            span = pl.ds(g * rows, rows)
            for q in range(pieces):
                at = slice(q * LANES, (q + 1) * LANES)
                rows_x[span, at] = found[q * rows : (q + 1) * rows]
                rows_dy[span, at] = found[(pieces + q) * rows : (pieces + q + 1) * rows]

    def cell(item):
        t, start, wide = item
        return slice(None), pl.ds(t * span_rows, span_rows), pl.ds(start, wide)

    def copy_a(i):
        at = cell(order[i])
        return pltpu.make_async_remote_copy(
            src_ref=send_a.at[at], dst_ref=recv_a.at[at], send_sem=a_send, recv_sem=a_recv.at[i % RING],
            device_id=(partner, e), device_id_type=MESH,
        )

    def copy_b(i, j):
        at = cell(order[i])
        to = lax.rem(x + j, n_x) * CORES + core
        return pltpu.make_async_remote_copy(
            src_ref=send_b.at[at], dst_ref=recv_b.at[(j - 1, *at)], send_sem=b_send, recv_sem=b_recv.at[i, j - 1],
            device_id=(to, e), device_id_type=MESH,
        )

    def copy_c(i):
        at = cell(order[i])
        return pltpu.make_async_remote_copy(
            src_ref=acts.at[at], dst_ref=recv_c.at[at], send_sem=c_send, recv_sem=c_recv.at[i % RING],
            device_id=(partner, e), device_id_type=MESH,
        )

    def columns(h, start, wide):
        return pl.ds(pl.multiple_of(h * half + start, LANES), wide)

    def group(t):
        return pl.ds(t * span_rows, span_rows)

    def partials(h, item):
        t, start, wide = item
        cols = columns(h, start, wide)
        xs, dys = rows_x[group(t)], rows_dy[group(t)]
        yield jnp.dot(xs, wg[:, cols], preferred_element_type=F32)
        yield jnp.dot(xs, wu[:, cols], preferred_element_type=F32)
        yield lax.dot_general(dys, wd[cols, :], LAST, preferred_element_type=F32)

    def stage1(i):
        _, rows_at, cols_at = cell(order[i])
        for n, v in enumerate(partials(1 - core, order[i])):
            send_a[n, rows_at, cols_at] = v.astype(BF16)
        copy_a(i).start()
        for n, v in enumerate(partials(core, order[i])):
            own_a[n, rows_at, cols_at] = v

    def stage2(i):
        at = cell(order[i])
        copy_a(i).wait_recv()
        v = own_a[at] + recv_a[at].astype(F32)
        own_a[at] = v
        send_b[at] = v.astype(BF16)
        for j in range(1, n_x):
            copy_b(i, j).start()

    def stage3(i):
        t, _, wide = order[i]
        _, rows_at, cols_at = cell(order[i])
        for j in range(1, n_x):
            copy_b(i, j).wait_recv()
        pre = []
        for n in range(3):
            v = own_a[n, rows_at, cols_at]
            for j in range(n_x - 1):
                v = v + recv_b[j, n, rows_at, cols_at].astype(F32)
            pre.append(v)
        gate_pre, up_pre, hidden_grad = pre
        sigma = jax.nn.sigmoid(gate_pre)
        active = gate_pre * sigma
        hidden = (active * up_pre).astype(BF16)
        acts[0, rows_at, cols_at] = (
            hidden_grad * up_pre * sigma * (1.0 + gate_pre * (1.0 - sigma))
        ).astype(BF16)
        acts[1, rows_at, cols_at] = (hidden_grad * active).astype(BF16)
        acts[2, rows_at, cols_at] = hidden
        copy_c(i).start()
        prod = hidden.astype(F32) * hidden_grad
        dot = sum(prod[:, p : p + LANES] for p in range(0, wide, LANES))
        dots[group(t)] = dot if i == opening[t] else dots[group(t)] + dot

    def grads(h, i, source):
        _, rows_at, cols_at = cell(order[i])
        cols = columns(h, *order[i][1:])
        part = lax.dot_general(source[0, rows_at, cols_at], wg[:, cols], LAST, preferred_element_type=F32)
        return part + lax.dot_general(source[1, rows_at, cols_at], wu[:, cols], LAST, preferred_element_type=F32)

    def weights(start, wide):
        at = pl.ds(start, wide)
        for h, source in ((core, acts), (1 - core, recv_c)):
            cols = columns(h, start, wide)
            xs, dys = rows_x[...], rows_dy[...]
            og[:, cols] = lax.dot_general(xs, source[0, :, at], FIRST, preferred_element_type=F32).astype(BF16)
            ou[:, cols] = lax.dot_general(xs, source[1, :, at], FIRST, preferred_element_type=F32).astype(BF16)
            od[cols, :] = lax.dot_general(source[2, :, at], dys, FIRST, preferred_element_type=F32).astype(BF16)

    def stage4(i):
        t = order[i][0]
        part = grads(core, i, acts)
        copy_c(i).wait_recv()
        part = part + grads(1 - core, i, recv_c)
        dx[group(t)] = part if i == opening[t] else dx[group(t)] + part

    opening = [next(i for i, item in enumerate(order) if item[0] == t) for t in range(GROUPS)]
    closing = [max(i for i, item in enumerate(order) if item[0] == t) for t in range(GROUPS)]
    n_items = len(order)
    for c in loads:
        c.wait()
    prepare(0)
    for i in range(n_items):
        if i == opening[1]:
            stage2(i - 1)
            prepare(1)
        stage1(i)
        if i > 0 and i != opening[1]:
            stage2(i - 1)
    stage2(n_items - 1)

    once = jnp.where(x == 0, 1.0, 0.0)
    mark = lax.rem(iota((grp * sub, LANES), 0), sub) == (pieces + 1) * CAP

    def give_back(t):
        for g in range(t * size // grp, (t + 1) * size // grp):
            span = pl.ds(g * grp * CAP, grp * CAP)
            grads = dx[span].astype(BF16)
            mine = jnp.sum(dots[span], axis=1, keepdims=True) * once
            mine = jnp.broadcast_to(mine, (grp * CAP, LANES)).astype(BF16)
            stack = [grads[:, q * LANES : (q + 1) * LANES] for q in range(pieces)] + [mine]
            back = jnp.dot(put[...], jnp.concatenate(stack, axis=0), preferred_element_type=F32)
            back = jnp.where(mark, counts, back).astype(BF16)
            send2[g * grp : (g + 1) * grp] = back.reshape(grp, sub, LANES)

        def give(g, b):
            pltpu.make_async_remote_copy(
                src_ref=send2.at[t * size + b * n_fsdp + g], dst_ref=recv2.at[me], send_sem=r_send, recv_sem=r_recv,
                device_id=(g, (other if t else half_of) * blocks + b), device_id_type=MESH,
            ).start()

        visit(give, t > 0)
        if t == 0:
            recv2[me] = send2[place]

    for i in range(n_items):
        if EARLY and i - 1 == closing[1]:
            stage4(i - 1)
            give_back(1)
        stage3(i)
        if i > 0 and not (EARLY and i - 1 == closing[1]):
            stage4(i - 1)
            if i - 1 == closing[1]:
                give_back(1)
    stage4(n_items - 1)
    if closing[1] == n_items - 1:
        give_back(1)
    give_back(0)
    block_w = min(half, 2 * LANES)
    for start in range(0, half, block_w):
        weights(start, block_w)
    everyone2 = recv2.at[pl.ds(0, n_dev - 1)]
    everyone = recv1.at[pl.ds(0, size - 1 + n_fsdp)]
    pltpu.make_async_copy(everyone, everyone, d_send).wait()
    if blocks > 1:
        passed = recv1.at[pl.ds(0, (blocks - 1) * n_fsdp)]
        pltpu.make_async_copy(passed, passed, s_send).wait()
    pltpu.make_async_copy(everyone2, everyone2, r_send).wait()
    for buffer, sem in ((send_a, a_send), (recv_b, b_send), (acts, c_send)):
        pltpu.make_async_copy(buffer, buffer, sem).wait()
    pltpu.make_async_copy(everyone2, everyone2, r_recv).wait()

    rest = jnp.zeros(((EXP_WIN + 1) * n_tok, LANES), F32)
    for g in range(n_fsdp):
        came = recv2[g * n_ep : (g + 1) * n_ep].reshape(reach, LANES)
        made = jnp.dot(final[...], came, preferred_element_type=F32)
        for q in range(pieces):
            at = g * depth + q * LANES
            gt_ref[:, at : at + LANES] = made[q * n_tok : (q + 1) * n_tok].astype(BF16)
        rest = rest + made[pieces * n_tok :]
    for k in range(EXP_WIN):
        col = rest[k * n_tok : (k + 1) * n_tok, 0:n_tok]
        rd_ref[k : k + 1, :] = jnp.sum(jnp.where(ti == tj, col, 0.0), axis=0, keepdims=True)
    count = rest[EXP_WIN * n_tok : EXP_WIN * n_tok + 1, 0:n_exp]
    target = n_exp * (count / (2 * n_tok * n_dev))
    aux_ref[...] = probs * (target - jnp.sum(probs * target, axis=1, keepdims=True))


def put_kernel(n, *refs):
    sources, targets, sem = refs[:n], refs[n : 2 * n], refs[2 * n]
    for i, (s, t) in enumerate(zip(sources, targets)):
        rows = s.shape[0]
        pieces = PIECES if rows % (16 * PIECES) == 0 else 1
        for p in range(pieces):
            span = pl.ds(p * (rows // pieces), rows // pieces)
            pltpu.make_async_copy(s.at[span], t.at[span], sem.at[i]).start()
    for i, (s, t) in enumerate(zip(sources, targets)):
        pltpu.make_async_copy(s, t, sem.at[i]).wait()


def body(n_fsdp, n_ep, tokens, cotangent, routes, logits, w_gate, w_up, w_down):
    n_tok, model = tokens.shape
    depth, width = w_gate.shape
    n_dev = n_fsdp * n_ep
    n_x = n_fsdp // CORES
    rows = n_dev * CAP
    half = width // CORES
    order = plan(half)
    items = len(order)
    pieces = depth // LANES
    sub = -(-((pieces + 1) * CAP + 1) // 8) * 8
    pack = -(-2 * CAP * pieces // 8) * 8
    grp = min(16, n_dev // EXP_WIN)
    vmem = pl.BlockSpec(memory_space=pltpu.VMEM)
    hbm = pl.BlockSpec(memory_space=pl.ANY)
    dma = pltpu.SemaphoreType.DMA
    made = (
        ((n_tok, model), BF16),
        ((EXP_WIN, n_tok), F32),
        (logits.shape, F32),
        (w_gate.shape, BF16),
        (w_up.shape, BF16),
        (w_down.shape, BF16),
    )
    held = pl.pallas_call(
        functools.partial(kernel, n_fsdp, n_ep, order, sub, pack),
        out_shape=tuple(pltpu.VMEM(d, t) for d, t in made),
        in_specs=[hbm] * 7,
        out_specs=[vmem] * 6,
        scratch_shapes=[
            pltpu.VMEM(tokens.shape, BF16),
            pltpu.VMEM(cotangent.shape, BF16),
            pltpu.VMEM(routes.shape[::-1], routes.dtype),
            pltpu.VMEM(logits.shape, F32),
            pltpu.VMEM(w_gate.shape, BF16),
            pltpu.VMEM(w_up.shape, BF16),
            pltpu.VMEM(w_down.shape, BF16),
            pltpu.VMEM((EXP_WIN, n_fsdp, pack, LANES), BF16),
            pltpu.VMEM((n_dev, pack, LANES), BF16),
            pltpu.VMEM((rows, depth), BF16),
            pltpu.VMEM((rows, depth), BF16),
            pltpu.VMEM((3, rows, half), F32),
            pltpu.VMEM((3, rows, half), BF16),
            pltpu.VMEM((3, rows, half), BF16),
            pltpu.VMEM((3, rows, half), BF16),
            pltpu.VMEM((n_x - 1, 3, rows, half), BF16),
            pltpu.VMEM((3, rows, half), BF16),
            pltpu.VMEM((3, rows, half), BF16),
            pltpu.VMEM((rows, depth), F32),
            pltpu.VMEM((rows, LANES), F32),
            pltpu.VMEM((n_dev, sub, LANES), BF16),
            pltpu.VMEM((n_dev, sub, LANES), BF16),
            pltpu.VMEM((grp * sub, (pieces + 1) * grp * CAP), BF16),
            pltpu.VMEM((2 * pieces * grp * CAP, grp * pack), BF16),
            pltpu.VMEM(((pieces + EXP_WIN + 1) * n_tok, n_ep * sub), BF16),
            dma((4,)),
            dma((3,)),
            dma,
            dma((GROUPS,)),
            dma,
            dma,
            dma,
            dma((RING,)),
            dma,
            dma((items, n_x - 1)),
            dma,
            dma((RING,)),
            dma,
            dma,
        ],
        compiler_params=pltpu.CompilerParams(
            collective_id=0, has_side_effects=True, vmem_limit_bytes=54 * 1024 * 1024
        ),
    )(tokens, cotangent, jnp.transpose(routes), logits, w_gate, w_up, w_down)
    out = pl.pallas_call(
        functools.partial(put_kernel, len(made)),
        out_shape=tuple(jax.ShapeDtypeStruct(d, t) for d, t in made),
        in_specs=[vmem] * len(made),
        out_specs=[hbm] * len(made),
        scratch_shapes=[dma((len(made),))],
        compiler_params=pltpu.CompilerParams(vmem_limit_bytes=1024 * 1024),
    )(*held)
    return (out[0], jnp.transpose(out[1])) + tuple(out[2:])


def solution(mesh):
    in_specs = (
        P(("fsdp", "ep"), None),
        P(("fsdp", "ep"), None),
        P(("fsdp", "ep"), None),
        P(("fsdp", "ep"), None),
        P("fsdp", "ep"),
        P("fsdp", "ep"),
        P("ep", "fsdp"),
    )
    out_specs = (
        P(("fsdp", "ep"), None),
        P(("fsdp", "ep"), None),
        P(("fsdp", "ep"), None),
        P("fsdp", "ep"),
        P("fsdp", "ep"),
        P("ep", "fsdp"),
    )
    step = functools.partial(body, mesh.shape["fsdp"], mesh.shape["ep"])
    return jax.shard_map(step, mesh=mesh, in_specs=in_specs, out_specs=out_specs, check_vma=False)
```

```python
import functools

import jax
import jax.numpy as jnp
from jax import lax
from jax.experimental import pallas as pl
from jax.experimental.pallas import tpu as pltpu
from jax.sharding import PartitionSpec as P

EXP_WIN = 2
CAP = 3
CORES = 2
FRONT = (1, 2, 2)
MIDDLE = (1, 2, 2, 2, 1)
BACK = (2, 1)
EARLY = True
GROUPS = EXP_WIN
LANES = 128
PIECES = 8
RING = 4
LAST = (((1,), (1,)), ((), ()))
FIRST = (((0,), (0,)), ((), ()))
F32 = jnp.float32
BF16 = jnp.bfloat16
MESH = pl.DeviceIdType.MESH


def iota(shape, axis):
    return lax.broadcasted_iota(jnp.int32, shape, axis)


def plan(half):
    if half % (8 * LANES):
        return ((0, 0, half), (1, 0, half))
    u = half // 8
    cuts = FRONT + BACK
    items = [(0, u * sum(cuts[:i]), u * c) for i, c in enumerate(cuts)]
    far = [(1, u * sum(MIDDLE[:i]), u * c) for i, c in enumerate(MIDDLE)]
    return (*items[: len(FRONT)], *far, *items[len(FRONT) :])


def kernel(
    n_fsdp, n_ep, order, sub, pack,
    tok_hbm, cot_hbm, routes_hbm, logits_hbm, wg_hbm, wu_hbm, wd_hbm,
    gt_ref, rd_ref, aux_ref, og, ou, od,
    tok_ref, cot_ref, routes_ref, logits_ref, wg, wu, wd,
    send1, recv1, rows_x, rows_dy,
    own_a, send_a, recv_a, send_b, recv_b, acts, recv_c, dx, dots, send2, recv2, put, pick, final,
    i_sem, w_sem, d_send, d_recv, s_send, s_recv, a_send, a_recv, b_send, b_recv, c_send, c_recv, r_send, r_recv,
):
    n_dev = n_fsdp * n_ep
    n_x = n_fsdp // CORES
    blocks = n_ep // EXP_WIN
    f, e = lax.axis_index("fsdp"), lax.axis_index("ep")
    me = f * n_ep + e
    x, core = f // CORES, lax.rem(f, CORES)
    partner = x * CORES + (1 - core)
    half_of, block = e // blocks, lax.rem(e, blocks)
    other = 1 - half_of
    depth, width = wg.shape
    half = width // CORES
    size = n_fsdp * blocks
    span_rows = size * CAP
    place = block * n_fsdp + f
    pieces = depth // LANES

    columns_f = [lax.rem(f + j, n_fsdp) for j in range(n_fsdp)]

    def visit(act, own):
        def row(j, first=0):
            b = lax.rem(block + j, blocks)
            for g in columns_f[first:]:
                act(g, b)

        if blocks <= 4:
            for j in range(1, blocks):
                row(j)
        else:
            lax.fori_loop(1, blocks, lambda j, _: (row(j), 0)[1], 0)
        row(0, 0 if own else 1)

    barrier = pltpu.get_barrier_semaphore()

    def greet(g, at):
        pl.semaphore_signal(barrier, inc=1, device_id=(g, at), device_id_type=MESH)

    for g in columns_f:
        greet(g, other * blocks + block)
    visit(lambda g, b: greet(g, half_of * blocks + b), False)
    smalls = [
        pltpu.make_async_copy(s, t, i_sem.at[i])
        for i, (s, t) in enumerate(
            ((routes_hbm, routes_ref), (logits_hbm, logits_ref), (tok_hbm, tok_ref), (cot_hbm, cot_ref))
        )
    ]
    for c in smalls:
        c.start()

    loads = [
        pltpu.make_async_copy(s, t, w_sem.at[i])
        for i, (s, t) in enumerate(((wg_hbm, wg), (wu_hbm, wu), (wd_hbm, wd)))
    ]
    for c in smalls:
        c.wait()
    for c in loads:
        c.start()

    routes = routes_ref[...]
    logits = logits_ref[...]
    n_tok, n_exp = logits.shape
    ti, tj = iota((n_tok, n_tok), 0), iota((n_tok, n_tok), 1)
    r0, r1 = (
        jnp.sum(jnp.where(ti == tj, routes[k : k + 1, :], 0), axis=1, keepdims=True) for k in range(2)
    )
    experts = iota((n_tok, n_exp), 1)
    c0 = jnp.sum(jnp.where(experts == r0, logits, 0.0), axis=1, keepdims=True)
    c1 = jnp.sum(jnp.where(experts == r1, logits, 0.0), axis=1, keepdims=True)
    top = jnp.maximum(c0, c1)
    e0, e1 = jnp.exp(c0 - top), jnp.exp(c1 - top)
    p0, p1 = e0 / (e0 + e1), e1 / (e0 + e1)
    spread = pieces * n_tok
    wi, wj = iota((pack, 2 * spread), 0), iota((pack, 2 * spread), 1)
    wq, wp = wi // (2 * CAP), lax.rem(wi, 2 * CAP)
    want = (wq == lax.rem(wj, spread) // n_tok) & (wp // CAP == wj // spread)
    slot_of = lax.rem(wp, CAP).astype(F32)
    ui, uj = iota((n_tok, 2 * spread), 0), lax.rem(iota((n_tok, 2 * spread), 1), n_tok)

    def cut(v):
        return jnp.concatenate(
            [
                jnp.concatenate(
                    [v[:, g * depth + q * LANES : g * depth + (q + 1) * LANES] for g in range(n_fsdp)], axis=1
                )
                for q in range(pieces)
            ],
            axis=0,
        )

    tok = cut(tok_ref[...].astype(F32))
    cot = cut(cot_ref[...].astype(F32))
    member_col, slot_col = [], []
    for k in range(EXP_WIN):
        m0, m1 = jnp.where(r0 == k, 1.0, 0.0), jnp.where(r1 == k, 1.0, 0.0)
        col = m0 + m1
        weight = m0 * p0 + m1 * p1
        mine = jnp.sum(jnp.where(ui == uj, col, 0.0), axis=0, keepdims=True)
        slot = jnp.sum(jnp.where(ui < uj, col, 0.0), axis=0, keepdims=True)
        row = jnp.sum(jnp.where(ti == tj, col, 0.0), axis=0, keepdims=True)
        slot_col.append(jnp.sum(jnp.where(tj < ti, row, 0.0), axis=1, keepdims=True))
        member_col.append(col)
        sel = jnp.where(want & (slot_of == slot), mine, 0.0).astype(BF16)
        weighted = cot * jnp.concatenate([weight] * pieces, axis=0)
        both = jnp.concatenate([tok, weighted], axis=0).astype(BF16)
        sent = jnp.dot(sel, both, preferred_element_type=F32).astype(BF16)
        for g in range(n_fsdp):
            send1[k, g] = sent[:, g * LANES : (g + 1) * LANES]

    pl.semaphore_wait(barrier, size - 1 + n_fsdp)

    def push(g, b):
        pltpu.make_async_remote_copy(
            src_ref=send1.at[half_of, g], dst_ref=recv1.at[place], send_sem=d_send, recv_sem=d_recv.at[0],
            device_id=(g, half_of * blocks + b), device_id_type=MESH,
        ).start()

    visit(push, False)
    for g in columns_f:
        pltpu.make_async_remote_copy(
            src_ref=send1.at[other, g], dst_ref=recv1.at[size + place],
            send_sem=d_send, recv_sem=d_recv.at[1], device_id=(g, other * blocks + block), device_id_type=MESH,
        ).start()
    recv1[place] = send1[half_of, f]

    shared = recv1.at[pl.ds(size + block * n_fsdp, n_fsdp)]

    def share(j):
        return pltpu.make_async_remote_copy(
            src_ref=shared, dst_ref=shared, send_sem=s_send, recv_sem=s_recv,
            device_id=(f, half_of * blocks + lax.rem(block + j, blocks)), device_id_type=MESH,
        )

    def relay():
        pltpu.make_async_copy(shared, shared, d_recv.at[1]).wait()

        if blocks <= 4:
            for j in range(1, blocks):
                share(j).start()
        else:
            lax.fori_loop(1, blocks, lambda j, _: (share(j).start(), 0)[1], 0)

    grp = min(8, size)
    lanes = iota((n_tok, LANES), 1)
    counts = jnp.sum(
        jnp.where(lanes == r0, 1.0, 0.0) + jnp.where(lanes == r1, 1.0, 0.0), axis=0, keepdims=True
    )
    raised = jnp.exp(logits - jnp.max(logits, axis=1, keepdims=True))
    probs = raised / jnp.sum(raised, axis=1, keepdims=True)
    put_shape = (grp * sub, (pieces + 1) * grp * CAP)
    pi, pj = iota(put_shape, 0), iota(put_shape, 1)
    pr = lax.rem(pj, grp * CAP)
    put[...] = jnp.where(
        (pi // sub == pr // CAP) & (lax.rem(pi, sub) == pj // (grp * CAP) * CAP + lax.rem(pr, CAP)), 1.0, 0.0
    ).astype(BF16)
    reach = n_ep * sub
    fj = iota((n_tok, reach), 1)
    fk, fs = fj // (blocks * sub), lax.rem(fj, sub).astype(F32)
    picks = []
    for q in range(pieces):
        row = jnp.zeros((n_tok, reach), F32)
        for k in range(EXP_WIN):
            row = row + jnp.where((fk == k) & (fs == slot_col[k] + q * CAP), member_col[k], 0.0)
        picks.append(row)
    for k in range(EXP_WIN):
        picks.append(jnp.where((fk == k) & (fs == slot_col[k] + pieces * CAP), member_col[k], 0.0))
    picks.append(jnp.where(fs == (pieces + 1) * CAP, 1.0, 0.0))
    final[...] = jnp.concatenate(picks, axis=0).astype(BF16)

    rows = grp * CAP
    pick_shape = (2 * pieces * rows, grp * pack)
    si, sj = iota(pick_shape, 0), iota(pick_shape, 1)
    sr, sb = lax.rem(si, rows), si // rows
    pick[...] = jnp.where(
        sj == sr // CAP * pack + lax.rem(sb, pieces) * 2 * CAP + sb // pieces * CAP + lax.rem(sr, CAP), 1.0, 0.0
    ).astype(BF16)

    def prepare(t):
        if t == 0:
            landed = recv1.at[pl.ds(0, size - 1)]
            pltpu.make_async_copy(landed, landed, d_recv.at[0]).wait()
            relay()
        elif blocks > 1:
            landed = recv1.at[pl.ds(0, (blocks - 1) * n_fsdp)]
            pltpu.make_async_copy(landed, landed, s_recv).wait()
        for g in range(t * size // grp, (t + 1) * size // grp):
            came = recv1[g * grp : (g + 1) * grp].reshape(grp * pack, LANES)
            found = jnp.dot(pick[...], came, preferred_element_type=F32).astype(BF16)
            span = pl.ds(g * rows, rows)
            for q in range(pieces):
                at = slice(q * LANES, (q + 1) * LANES)
                rows_x[span, at] = found[q * rows : (q + 1) * rows]
                rows_dy[span, at] = found[(pieces + q) * rows : (pieces + q + 1) * rows]

    def cell(item):
        t, start, wide = item
        return slice(None), pl.ds(t * span_rows, span_rows), pl.ds(start, wide)

    def copy_a(i):
        at = cell(order[i])
        return pltpu.make_async_remote_copy(
            src_ref=send_a.at[at], dst_ref=recv_a.at[at], send_sem=a_send, recv_sem=a_recv.at[i % RING],
            device_id=(partner, e), device_id_type=MESH,
        )

    def copy_b(i, j):
        at = cell(order[i])
        to = lax.rem(x + j, n_x) * CORES + core
        return pltpu.make_async_remote_copy(
            src_ref=send_b.at[at], dst_ref=recv_b.at[(j - 1, *at)], send_sem=b_send, recv_sem=b_recv.at[i, j - 1],
            device_id=(to, e), device_id_type=MESH,
        )

    def copy_c(i):
        at = cell(order[i])
        return pltpu.make_async_remote_copy(
            src_ref=acts.at[at], dst_ref=recv_c.at[at], send_sem=c_send, recv_sem=c_recv.at[i % RING],
            device_id=(partner, e), device_id_type=MESH,
        )

    def columns(h, start, wide):
        return pl.ds(pl.multiple_of(h * half + start, LANES), wide)

    def group(t):
        return pl.ds(t * span_rows, span_rows)

    def partials(h, item):
        t, start, wide = item
        cols = columns(h, start, wide)
        xs, dys = rows_x[group(t)], rows_dy[group(t)]
        yield jnp.dot(xs, wg[:, cols], preferred_element_type=F32)
        yield jnp.dot(xs, wu[:, cols], preferred_element_type=F32)
        yield lax.dot_general(dys, wd[cols, :], LAST, preferred_element_type=F32)

    def stage1(i):
        _, rows_at, cols_at = cell(order[i])
        for n, v in enumerate(partials(1 - core, order[i])):
            send_a[n, rows_at, cols_at] = v.astype(BF16)
        copy_a(i).start()
        for n, v in enumerate(partials(core, order[i])):
            own_a[n, rows_at, cols_at] = v

    def stage2(i):
        at = cell(order[i])
        copy_a(i).wait_recv()
        v = own_a[at] + recv_a[at].astype(F32)
        own_a[at] = v
        send_b[at] = v.astype(BF16)
        for j in range(1, n_x):
            copy_b(i, j).start()

    def stage3(i):
        t, _, wide = order[i]
        _, rows_at, cols_at = cell(order[i])
        for j in range(1, n_x):
            copy_b(i, j).wait_recv()
        pre = []
        for n in range(3):
            v = own_a[n, rows_at, cols_at]
            for j in range(n_x - 1):
                v = v + recv_b[j, n, rows_at, cols_at].astype(F32)
            pre.append(v)
        gate_pre, up_pre, hidden_grad = pre
        sigma = jax.nn.sigmoid(gate_pre)
        active = gate_pre * sigma
        hidden = (active * up_pre).astype(BF16)
        acts[0, rows_at, cols_at] = (
            hidden_grad * up_pre * sigma * (1.0 + gate_pre * (1.0 - sigma))
        ).astype(BF16)
        acts[1, rows_at, cols_at] = (hidden_grad * active).astype(BF16)
        acts[2, rows_at, cols_at] = hidden
        copy_c(i).start()
        prod = hidden.astype(F32) * hidden_grad
        dot = sum(prod[:, p : p + LANES] for p in range(0, wide, LANES))
        dots[group(t)] = dot if i == opening[t] else dots[group(t)] + dot

    def grads(h, i, source):
        _, rows_at, cols_at = cell(order[i])
        cols = columns(h, *order[i][1:])
        part = lax.dot_general(source[0, rows_at, cols_at], wg[:, cols], LAST, preferred_element_type=F32)
        return part + lax.dot_general(source[1, rows_at, cols_at], wu[:, cols], LAST, preferred_element_type=F32)

    def weights(start, wide):
        at = pl.ds(start, wide)
        for h, source in ((core, acts), (1 - core, recv_c)):
            cols = columns(h, start, wide)
            xs, dys = rows_x[...], rows_dy[...]
            og[:, cols] = lax.dot_general(xs, source[0, :, at], FIRST, preferred_element_type=F32).astype(BF16)
            ou[:, cols] = lax.dot_general(xs, source[1, :, at], FIRST, preferred_element_type=F32).astype(BF16)
            od[cols, :] = lax.dot_general(source[2, :, at], dys, FIRST, preferred_element_type=F32).astype(BF16)

    def stage4(i):
        t = order[i][0]
        part = grads(core, i, acts)
        copy_c(i).wait_recv()
        part = part + grads(1 - core, i, recv_c)
        dx[group(t)] = part if i == opening[t] else dx[group(t)] + part

    opening = [next(i for i, item in enumerate(order) if item[0] == t) for t in range(GROUPS)]
    closing = [max(i for i, item in enumerate(order) if item[0] == t) for t in range(GROUPS)]
    n_items = len(order)
    for c in loads:
        c.wait()
    prepare(0)
    for i in range(n_items):
        if i == opening[1]:
            stage2(i - 1)
            prepare(1)
        stage1(i)
        if i > 0 and i != opening[1]:
            stage2(i - 1)
    stage2(n_items - 1)

    once = jnp.where(x == 0, 1.0, 0.0)
    mark = lax.rem(iota((grp * sub, LANES), 0), sub) == (pieces + 1) * CAP

    def give_back(t):
        for g in range(t * size // grp, (t + 1) * size // grp):
            span = pl.ds(g * grp * CAP, grp * CAP)
            grads = dx[span].astype(BF16)
            mine = jnp.sum(dots[span], axis=1, keepdims=True) * once
            mine = jnp.broadcast_to(mine, (grp * CAP, LANES)).astype(BF16)
            stack = [grads[:, q * LANES : (q + 1) * LANES] for q in range(pieces)] + [mine]
            back = jnp.dot(put[...], jnp.concatenate(stack, axis=0), preferred_element_type=F32)
            back = jnp.where(mark, counts, back).astype(BF16)
            send2[g * grp : (g + 1) * grp] = back.reshape(grp, sub, LANES)

        def give(g, b):
            pltpu.make_async_remote_copy(
                src_ref=send2.at[t * size + b * n_fsdp + g], dst_ref=recv2.at[me], send_sem=r_send, recv_sem=r_recv,
                device_id=(g, (other if t else half_of) * blocks + b), device_id_type=MESH,
            ).start()

        visit(give, t > 0)
        if t == 0:
            recv2[me] = send2[place]

    for i in range(n_items):
        if EARLY and i - 1 == closing[1]:
            stage4(i - 1)
            give_back(1)
        stage3(i)
        if i > 0 and not (EARLY and i - 1 == closing[1]):
            stage4(i - 1)
            if i - 1 == closing[1]:
                give_back(1)
    stage4(n_items - 1)
    if closing[1] == n_items - 1:
        give_back(1)
    give_back(0)
    block_w = min(half, 2 * LANES)
    for start in range(0, half, block_w):
        weights(start, block_w)
    everyone2 = recv2.at[pl.ds(0, n_dev - 1)]
    everyone = recv1.at[pl.ds(0, size - 1 + n_fsdp)]
    pltpu.make_async_copy(everyone, everyone, d_send).wait()
    if blocks > 1:
        passed = recv1.at[pl.ds(0, (blocks - 1) * n_fsdp)]
        pltpu.make_async_copy(passed, passed, s_send).wait()
    pltpu.make_async_copy(everyone2, everyone2, r_send).wait()
    for buffer, sem in ((send_a, a_send), (recv_b, b_send), (acts, c_send)):
        pltpu.make_async_copy(buffer, buffer, sem).wait()
    pltpu.make_async_copy(everyone2, everyone2, r_recv).wait()

    rest = jnp.zeros(((EXP_WIN + 1) * n_tok, LANES), F32)
    for g in range(n_fsdp):
        came = recv2[g * n_ep : (g + 1) * n_ep].reshape(reach, LANES)
        made = jnp.dot(final[...], came, preferred_element_type=F32)
        for q in range(pieces):
            at = g * depth + q * LANES
            gt_ref[:, at : at + LANES] = made[q * n_tok : (q + 1) * n_tok].astype(BF16)
        rest = rest + made[pieces * n_tok :]
    for k in range(EXP_WIN):
        col = rest[k * n_tok : (k + 1) * n_tok, 0:n_tok]
        rd_ref[k : k + 1, :] = jnp.sum(jnp.where(ti == tj, col, 0.0), axis=0, keepdims=True)
    count = rest[EXP_WIN * n_tok : EXP_WIN * n_tok + 1, 0:n_exp]
    target = n_exp * (count / (2 * n_tok * n_dev))
    aux_ref[...] = probs * (target - jnp.sum(probs * target, axis=1, keepdims=True))


def put_kernel(n, *refs):
    sources, targets, sem = refs[:n], refs[n : 2 * n], refs[2 * n]
    for i, (s, t) in enumerate(zip(sources, targets)):
        rows = s.shape[0]
        pieces = PIECES if rows % (16 * PIECES) == 0 else 1
        for p in range(pieces):
            span = pl.ds(p * (rows // pieces), rows // pieces)
            pltpu.make_async_copy(s.at[span], t.at[span], sem.at[i]).start()
    for i, (s, t) in enumerate(zip(sources, targets)):
        pltpu.make_async_copy(s, t, sem.at[i]).wait()


def body(n_fsdp, n_ep, tokens, cotangent, routes, logits, w_gate, w_up, w_down):
    n_tok, model = tokens.shape
    depth, width = w_gate.shape
    n_dev = n_fsdp * n_ep
    n_x = n_fsdp // CORES
    rows = n_dev * CAP
    half = width // CORES
    order = plan(half)
    items = len(order)
    pieces = depth // LANES
    sub = -(-((pieces + 1) * CAP + 1) // 8) * 8
    pack = -(-2 * CAP * pieces // 8) * 8
    grp = min(8, n_dev // EXP_WIN)
    vmem = pl.BlockSpec(memory_space=pltpu.VMEM)
    hbm = pl.BlockSpec(memory_space=pl.ANY)
    dma = pltpu.SemaphoreType.DMA
    made = (
        ((n_tok, model), BF16),
        ((EXP_WIN, n_tok), F32),
        (logits.shape, F32),
        (w_gate.shape, BF16),
        (w_up.shape, BF16),
        (w_down.shape, BF16),
    )
    held = pl.pallas_call(
        functools.partial(kernel, n_fsdp, n_ep, order, sub, pack),
        out_shape=tuple(pltpu.VMEM(d, t) for d, t in made),
        in_specs=[hbm] * 7,
        out_specs=[vmem] * 6,
        scratch_shapes=[
            pltpu.VMEM(tokens.shape, BF16),
            pltpu.VMEM(cotangent.shape, BF16),
            pltpu.VMEM(routes.shape[::-1], routes.dtype),
            pltpu.VMEM(logits.shape, F32),
            pltpu.VMEM(w_gate.shape, BF16),
            pltpu.VMEM(w_up.shape, BF16),
            pltpu.VMEM(w_down.shape, BF16),
            pltpu.VMEM((EXP_WIN, n_fsdp, pack, LANES), BF16),
            pltpu.VMEM((n_dev, pack, LANES), BF16),
            pltpu.VMEM((rows, depth), BF16),
            pltpu.VMEM((rows, depth), BF16),
            pltpu.VMEM((3, rows, half), F32),
            pltpu.VMEM((3, rows, half), BF16),
            pltpu.VMEM((3, rows, half), BF16),
            pltpu.VMEM((3, rows, half), BF16),
            pltpu.VMEM((n_x - 1, 3, rows, half), BF16),
            pltpu.VMEM((3, rows, half), BF16),
            pltpu.VMEM((3, rows, half), BF16),
            pltpu.VMEM((rows, depth), F32),
            pltpu.VMEM((rows, LANES), F32),
            pltpu.VMEM((n_dev, sub, LANES), BF16),
            pltpu.VMEM((n_dev, sub, LANES), BF16),
            pltpu.VMEM((grp * sub, (pieces + 1) * grp * CAP), BF16),
            pltpu.VMEM((2 * pieces * grp * CAP, grp * pack), BF16),
            pltpu.VMEM(((pieces + EXP_WIN + 1) * n_tok, n_ep * sub), BF16),
            dma((4,)),
            dma((3,)),
            dma,
            dma((GROUPS,)),
            dma,
            dma,
            dma,
            dma((RING,)),
            dma,
            dma((items, n_x - 1)),
            dma,
            dma((RING,)),
            dma,
            dma,
        ],
        compiler_params=pltpu.CompilerParams(
            collective_id=0, has_side_effects=True, vmem_limit_bytes=54 * 1024 * 1024
        ),
    )(tokens, cotangent, jnp.transpose(routes), logits, w_gate, w_up, w_down)
    out = pl.pallas_call(
        functools.partial(put_kernel, len(made)),
        out_shape=tuple(jax.ShapeDtypeStruct(d, t) for d, t in made),
        in_specs=[vmem] * len(made),
        out_specs=[hbm] * len(made),
        scratch_shapes=[dma((len(made),))],
        compiler_params=pltpu.CompilerParams(vmem_limit_bytes=1024 * 1024),
    )(*held)
    return (out[0], jnp.transpose(out[1])) + tuple(out[2:])


def solution(mesh):
    in_specs = (
        P(("fsdp", "ep"), None),
        P(("fsdp", "ep"), None),
        P(("fsdp", "ep"), None),
        P(("fsdp", "ep"), None),
        P("fsdp", "ep"),
        P("fsdp", "ep"),
        P("ep", "fsdp"),
    )
    out_specs = (
        P(("fsdp", "ep"), None),
        P(("fsdp", "ep"), None),
        P(("fsdp", "ep"), None),
        P("fsdp", "ep"),
        P("fsdp", "ep"),
        P("ep", "fsdp"),
    )
    step = functools.partial(body, mesh.shape["fsdp"], mesh.shape["ep"])
    return jax.shard_map(step, mesh=mesh, in_specs=in_specs, out_specs=out_specs, check_vma=False)
```
